32 devices in a mesh: dp: 8 (over z, x), expert: 4 (over y, core).
Axes of the slice: x: 2, y: 2, z: 4, core: 2. Of those that a mesh axis runs over, the one named last changes fastest.
Arguments:
- tokens: bfloat16 [1024, 4096], P('expert', 'dp'), may hold values from -6 to 6
- cotangent: bfloat16 [1024, 4096], P('expert', 'dp'), may hold values from -6 to 6
- expert_ids: int32 [1024, 2], P('expert'), may hold values from 0 to 3, all different within a row; in each aligned block of 256 rows (0 to 255, 256 to 511, ...) at most 129 rows name the same one
- combine: float32 [1024, 2], P('expert'), may hold values from 0.1 to 1
- w_gate: bfloat16 [4, 4096, 14336], P('expert', None, 'dp'), may hold values from -0.09375 to 0.09375
- w_up: bfloat16 [4, 4096, 14336], P('expert', None, 'dp'), may hold values from -0.09375 to 0.09375
- w_down: bfloat16 [4, 14336, 4096], P('expert', 'dp'), may hold values from -0.046875 to 0.046875
- scale_vector: float32 [4, 14336], P('expert', 'dp'), may hold values from 0.25 to 1.75
Outputs:
- token_grads: bfloat16 [1024, 4096], P('expert', 'dp')
- scale_grads: float32 [4, 14336], P('expert', 'dp')
The draws below stay inside these ranges and needn't reach their ends.
Inputs may be any that keep to these rules, and one draw needn't show every extreme that they name: `expert_ids`: each row names 2 different experts. Among the 256 rows of one aligned block no expert is named more than 129 times, and some block names some expert exactly 129 times.
All inputs are finite; a program needn't handle non-finite values.
Results may differ from the reference program's by a relative error of at most 0.0065.
Values may be sent and summed in bfloat16 or wider, within the bound.
A program may use at most 128 MiB of HBM per device.

```python
import math
import jax
import jax.numpy as jnp
import numpy as np
from jax import lax

D = 4096
FF = 14336
TOP = 2
TOK_DEV = 256
EXPERTS = 4
CAP = 129
TOKENS = 1024


def block_levels(rng, dims, cuts, low, high):
    def one(position, parts):
        heights = jax.random.uniform(jax.random.fold_in(jax.random.fold_in(rng, 6), position), (parts,), jnp.float32, low / len(cuts), high / len(cuts))
        return jnp.repeat(jnp.exp(heights), dims[position] // parts).reshape((-1,) + (1,) * (len(dims) - position - 1))

    loudness = one(*cuts[0])
    for cut in cuts[1:]:
        loudness = loudness * one(*cut)
    return loudness


def routed_block(rng, own, number, rows, number_of, top, most, skew):
    order = jax.random.permutation(rng, number_of)
    crowded, common = load_shares(number_of, rows * top, most, skew, True), load_shares(number_of, rows * top, most, skew, False)
    places = jnp.arange(number_of)

    def named(sizes, offset_by):
        used = int((sizes > 0).sum())
        fixed = max(1, used // 4)
        moved = fixed + (places - fixed + offset_by * (used - fixed)) % max(1, number_of - fixed)
        return jnp.zeros((number_of,), jnp.int32).at[order[jnp.where(places < fixed, places, moved)]].set(jnp.asarray(sizes, jnp.int32))

    sizes = jnp.where(number % 4 == 0, named(crowded, number // 4), named(common, number - number // 4 - 1))
    mixed = jax.random.permutation(jax.random.fold_in(own, 3), number_of)
    giver, sink = mixed[0:number_of // 2 * 2:2], mixed[1:number_of // 2 * 2:2]
    margin = jnp.minimum(sizes[giver] - 1, most - sizes[sink]) // 2
    margin = jnp.where((giver == order[0]) | (sink == order[0]) | (sizes[sink] == 0), 0, jnp.maximum(margin, 0))
    moved = jax.random.randint(jax.random.fold_in(own, 4), (number_of // 2,), 0, 1 << 20) % (margin + 1)
    sizes = sizes.at[giver].add(-moved).at[sink].add(moved)
    items = jnp.searchsorted(jnp.cumsum(sizes), jnp.arange(rows * top), side="right").astype(jnp.int32)
    listing = items.reshape(top, rows).T
    listing = listing[jax.random.permutation(jax.random.fold_in(own, 1), rows)]
    offset_by = jax.random.randint(jax.random.fold_in(own, 2), (rows, 1), 0, top)
    return jnp.take_along_axis(listing, (jnp.arange(top)[None, :] + offset_by) % top, axis=1)


def load_shares(number_of, total, limit, skew, full):
    weights = [(1 << 20) // math.isqrt(grade ** skew) + 1 for grade in range(1, number_of + 1)]
    largest = limit if full else min(limit, max(-(-total // number_of), total * weights[0] // sum(weights)))
    least = 1 if total - largest >= number_of - 1 else 0
    holding, surplus = [largest] + [least] * (number_of - 1), total - largest - least * (number_of - 1)
    while surplus > 0:
        free = [i for i in range(1, number_of) if holding[i] < largest] or [i for i in range(1, number_of) if holding[i] < limit]
        pool, left = sum([weights[i] for i in free]), surplus
        for i in free:
            extra = min(limit - holding[i], max(1, left * weights[i] // pool), surplus)
            holding[i] = holding[i] + extra
            surplus = surplus - extra
    return np.array(holding)


def gaussian(key, shape, deviation, bound, split=(), kind=jnp.bfloat16):
    result = jax.random.normal(key, shape, jnp.float32) * deviation
    if len(split) > 0:
        result = block_levels(key, shape, split, -0.22, 0.18) * result
    return jnp.clip(result, min=-bound, max=bound).astype(kind)


def setup_inputs(seed: int = 0) -> dict:
    streams_of = jax.random.split(jax.random.key(seed), 9)
    tokens = gaussian(streams_of[0], (TOKENS, D), 1.0, 6.0, ((0, 4), (1, 8)))
    cotangent = gaussian(streams_of[1], (TOKENS, D), 1.0, 6.0, ((0, 4), (1, 8)))
    expert_ids_keys = jax.random.split(jax.random.fold_in(streams_of[2], 1), TOKENS // TOK_DEV)
    expert_ids_turns = jax.random.permutation(jax.random.fold_in(streams_of[2], 3), TOKENS // TOK_DEV)
    expert_ids = jax.vmap(lambda own, number: routed_block(jax.random.fold_in(streams_of[2], 2), own, number, TOK_DEV, EXPERTS, TOP, CAP, 2))(expert_ids_keys, expert_ids_turns).reshape((TOKENS, TOP))
    combine = jnp.clip(0.1 + 0.9 * jax.random.uniform(streams_of[3], (TOKENS, TOP), jnp.float32) ** block_levels(streams_of[3], (TOKENS, TOP), ((0, 4),), -0.2, 0.2), 0.1, 1.0)
    w_gate = gaussian(streams_of[4], (EXPERTS, D, FF), D ** -0.5, 0.09375, ((0, 4), (2, 8)))
    w_up = gaussian(streams_of[5], (EXPERTS, D, FF), D ** -0.5, 0.09375, ((0, 4), (2, 8)))
    w_down = gaussian(streams_of[6], (EXPERTS, FF, D), FF ** -0.5, 0.046875, ((0, 4), (1, 8)))
    scale_vector = jnp.clip(1.0 + 0.15 * jax.random.normal(streams_of[7], (EXPERTS, FF), jnp.float32), 0.25, 1.75)
    return dict(tokens=tokens, cotangent=cotangent, expert_ids=expert_ids, combine=combine, w_gate=w_gate, w_up=w_up, w_down=w_down, scale_vector=scale_vector)


def route_tables(expert_ids, combine, experts, capacity):
    blocks = expert_ids.shape[0]
    per_block = expert_ids.shape[1]
    onehot = (expert_ids[:, :, :, None] == jnp.arange(experts, dtype=jnp.int32)).astype(jnp.int32)
    flat_hits = onehot.reshape(blocks, per_block * 2, experts)
    earlier = jnp.cumsum(flat_hits, axis=1) - flat_hits
    slot_ids = jnp.sum(earlier * flat_hits, axis=2).reshape(blocks, per_block, 2)
    positions = (slot_ids[:, :, :, None] == jnp.arange(capacity, dtype=jnp.int32)).astype(jnp.float32)
    matches = onehot.astype(jnp.float32)[:, :, :, :, None] * positions[:, :, :, None, :]
    dispatch = jnp.transpose(jnp.sum(matches, axis=2), (0, 2, 3, 1))
    slot_weight = jnp.sum(matches * combine[:, :, :, None, None], axis=(1, 2))
    return dispatch, slot_weight


def expert_backward(expert_items):
    rows_in, grads_in, gate_w, up_w, down_w, scale_vec = expert_items
    gate_act = jnp.dot(rows_in, gate_w, preferred_element_type=jnp.float32)
    up_act = jnp.dot(rows_in, up_w, preferred_element_type=jnp.float32)
    sigmoid_gate = jax.nn.sigmoid(gate_act)
    silu_gate = gate_act * sigmoid_gate
    hidden_grad = jnp.dot(grads_in, down_w.T, preferred_element_type=jnp.float32)
    scale_grad = jnp.sum(hidden_grad * silu_gate * up_act, axis=0)
    scaled_grad = hidden_grad * scale_vec
    up_grad = (scaled_grad * silu_gate).astype(jnp.bfloat16)
    gate_grad = (scaled_grad * up_act * sigmoid_gate * (1.0 + gate_act * (1.0 - sigmoid_gate))).astype(jnp.bfloat16)
    input_rows = jnp.dot(gate_grad, gate_w.T, preferred_element_type=jnp.float32) + jnp.dot(up_grad, up_w.T, preferred_element_type=jnp.float32)
    return scale_grad, input_rows


def reference(tokens, cotangent, expert_ids, combine, w_gate, w_up, w_down, scale_vector):
    blocks = TOKENS // TOK_DEV
    dispatch, slot_weight = route_tables(expert_ids.reshape(blocks, TOK_DEV, 2), combine.reshape(blocks, TOK_DEV, 2), EXPERTS, CAP)
    token_blocks = tokens.astype(jnp.float32).reshape(blocks, TOK_DEV, D)
    cot_blocks = cotangent.astype(jnp.float32).reshape(blocks, TOK_DEV, D)
    sent_rows = jnp.einsum('bect,btd->becd', dispatch, token_blocks, precision=lax.Precision.HIGHEST).astype(jnp.bfloat16)
    cot_rows = jnp.einsum('bect,btd->becd', dispatch, cot_blocks, precision=lax.Precision.HIGHEST)
    sent_grads = (slot_weight[:, :, :, None] * cot_rows).astype(jnp.bfloat16)
    rows_by_expert = jnp.moveaxis(sent_rows, 1, 0).reshape(EXPERTS, blocks * CAP, D)
    grads_by_expert = jnp.moveaxis(sent_grads, 1, 0).reshape(EXPERTS, blocks * CAP, D)
    scale_grads, input_rows = lax.map(expert_backward, (rows_by_expert, grads_by_expert, w_gate, w_up, w_down, scale_vector))
    input_rows = jnp.moveaxis(input_rows.reshape(EXPERTS, blocks, CAP, D), 0, 1)
    token_grads = jnp.einsum('bect,becd->btd', dispatch, input_rows, precision=lax.Precision.HIGHEST)
    return token_grads.reshape(TOKENS, D).astype(jnp.bfloat16), scale_grads
```

```python
import functools

import jax
import jax.numpy as jnp
from jax import lax
from jax.experimental import pallas as pl
from jax.experimental.pallas import tpu as pltpu
from jax.sharding import PartitionSpec as P


def route_tables(expert_ids, combine, experts, capacity):
    blocks = expert_ids.shape[0]
    per_block = expert_ids.shape[1]
    onehot = (expert_ids[:, :, :, None] == jnp.arange(experts, dtype=jnp.int32)).astype(jnp.int32)
    flat_hits = onehot.reshape(blocks, per_block * 2, experts)
    earlier = jnp.cumsum(flat_hits, axis=1) - flat_hits
    slot_ids = jnp.sum(earlier * flat_hits, axis=2).reshape(blocks, per_block, 2)
    positions = (slot_ids[:, :, :, None] == jnp.arange(capacity, dtype=jnp.int32)).astype(
        jnp.float32
    )
    matches = onehot.astype(jnp.float32)[:, :, :, :, None] * positions[:, :, :, None, :]
    dispatch = jnp.transpose(jnp.sum(matches, axis=2), (0, 2, 3, 1))
    slot_weight = jnp.sum(matches * combine[:, :, :, None, None], axis=(1, 2))
    return (dispatch, slot_weight, slot_ids)


def combine_slots(slot_table, flat_index):
    tok_count = flat_index.shape[0]
    picked = jnp.take(slot_table, flat_index.reshape(-1), axis=0).reshape(
        tok_count, 2, slot_table.shape[1]
    )
    return picked[:, 0].astype(jnp.float32) + picked[:, 1].astype(jnp.float32)


MESH = pl.DeviceIdType.MESH
ROW_TILE = 16
SHORT_RING = 8
VMEM_LIMIT = 60 * 1024 * 1024


def ring_order(mesh):
    count = mesh.shape["dp"]
    devices = mesh.devices.reshape(count, -1)[:, 0]
    places = {}
    for index, device in enumerate(devices):
        coords = getattr(device, "coords", None)
        if coords is None:
            return tuple(range(count))
        places[(coords[2], coords[0])] = index
    zs = sorted({z for z, _ in places})
    xs = sorted({x for _, x in places})
    if len(places) != count or len(zs) * len(xs) != count or len(zs) % 2 or len(xs) < 2:
        return tuple(range(count))
    order = [places[(z, xs[0])] for z in zs]
    for turn, z in enumerate(reversed(zs)):
        order += [places[(z, x)] for x in (xs[1:] if turn % 2 == 0 else xs[:0:-1])]
    return tuple(order)


def lookup(table, key):
    found = jnp.int32(table[0])
    for index in range(1, len(table)):
        found = jnp.where(key == index, jnp.int32(table[index]), found)
    return found


def ring_place(ring):
    n = len(ring)
    position_of = [0] * n
    for position, index in enumerate(ring):
        position_of[index] = position
    position = lookup(position_of, lax.axis_index("dp"))
    right = lookup(ring, lax.rem(position + 1, n))
    left = lookup(ring, lax.rem(position + n - 1, n))
    return position, right, left


def greet(right, left):
    barrier = pltpu.get_barrier_semaphore()
    for neighbour in (left, right):
        pl.semaphore_signal(barrier, inc=1, device_id={"dp": neighbour}, device_id_type=MESH)
    pl.semaphore_wait(barrier, 2)


def gather_kernel(
    ring, tile, x_ref, gate_w, up_w, gate_ref, up_ref, grads_ref, rows_ref, w_buf, w_sem, own_sem,
    send_sem, recv_sem,
):
    n = len(ring)
    width = x_ref.shape[1] // 2
    rows = x_ref.shape[0]
    cut = rows // 2 // ROW_TILE * ROW_TILE
    tiles = gate_w.shape[1] // tile
    position, right, left = ring_place(ring)
    me = lax.axis_index("dp")
    halves = (pl.ds(0, cut), pl.ds(cut, rows - cut))

    def tile_columns(t):
        return pl.ds(0, tile) if tiles == 1 else pl.ds(pl.multiple_of(t * tile, tile), tile)

    def load(t, slot):
        columns = tile_columns(t)
        return (
            pltpu.make_async_copy(gate_w.at[:, columns], w_buf.at[slot, 0], w_sem.at[slot, 0]),
            pltpu.make_async_copy(up_w.at[:, columns], w_buf.at[slot, 1], w_sem.at[slot, 1]),
        )

    for copy in load(0, 0):
        copy.start()

    def columns_of(index):
        return pl.ds(pl.multiple_of(index * width, width), width)

    for which, full in enumerate((rows_ref, grads_ref)):
        own = pltpu.make_async_copy(
            x_ref.at[:, pl.ds(which * width, width)], full.at[:, columns_of(me)], own_sem.at[which]
        )
        own.start()
        own.wait()
    greet(right, left)

    def hop(which, step, way):
        full = (rows_ref, grads_ref)[which]
        shift = n - step if way == 0 else step
        origin = lookup(ring, lax.rem(position + shift, n))
        spot = full.at[halves[way], columns_of(origin)]
        return pltpu.make_async_remote_copy(
            src_ref=spot,
            dst_ref=spot,
            send_sem=send_sem.at[which, way, step],
            recv_sem=recv_sem.at[which, way, step],
            device_id={"dp": right if way == 0 else left},
            device_id_type=MESH,
        )

    def advance(which, step):
        for way in range(2):

            @pl.when(step > 0)
            def _():
                hop(which, step - 1, way).wait_recv()

            hop(which, step, way).start()

    def rows_step(step, carry):
        advance(0, step)
        return carry

    lax.fori_loop(0, n - 1, rows_step, 0)
    for way in range(2):
        hop(1, 0, way).start()
    for way in range(2):
        hop(0, n - 2, way).wait_recv()

    def grads_step(step, carry):
        @pl.when(step > 0)
        def _():
            advance(1, step)

        @pl.when(step < tiles)
        def _():
            slot = lax.rem(step, 2)

            @pl.when(step + 1 < tiles)
            def _():
                for copy in load(step + 1, lax.rem(step + 1, 2)):
                    copy.start()

            columns = tile_columns(step)
            for copy in load(step, slot):
                copy.wait()
            gate_ref[:, columns] = jnp.dot(
                rows_ref[...], w_buf[slot, 0], preferred_element_type=jnp.float32
            )
            up_ref[:, columns] = jnp.dot(
                rows_ref[...], w_buf[slot, 1], preferred_element_type=jnp.float32
            )

        return carry

    lax.fori_loop(0, n - 1, grads_step, 0)
    for way in range(2):
        hop(1, n - 2, way).wait_recv()

    def finish(step, carry):
        for which in range(2):
            for way in range(2):
                hop(which, step, way).wait_send()
        return carry

    lax.fori_loop(0, n - 1, finish, 0)


def gather_acts(ring, x, gate_w, up_w):
    n = len(ring)
    rows, width = x.shape[0], x.shape[1] // 2
    hidden = gate_w.shape[1]
    tile = 256 if hidden % 256 == 0 and hidden // 256 <= n - 1 else hidden
    full = n * width
    vmem = pl.BlockSpec(memory_space=pltpu.VMEM)
    anywhere = pl.BlockSpec(memory_space=pl.ANY)
    return pl.pallas_call(
        functools.partial(gather_kernel, ring, tile),
        out_shape=(
            jax.ShapeDtypeStruct((rows, hidden), jnp.float32),
            jax.ShapeDtypeStruct((rows, hidden), jnp.float32),
            jax.ShapeDtypeStruct((rows, full), jnp.bfloat16),
        ),
        in_specs=[anywhere, anywhere, anywhere],
        out_specs=(vmem, vmem, vmem),
        scratch_shapes=[
            pltpu.VMEM((rows, full), jnp.bfloat16),
            pltpu.VMEM((2, 2, full, tile), jnp.bfloat16),
            pltpu.SemaphoreType.DMA((2, 2)),
            pltpu.SemaphoreType.DMA((2,)),
            pltpu.SemaphoreType.DMA((2, 2, n - 1)),
            pltpu.SemaphoreType.DMA((2, 2, n - 1)),
        ],
        compiler_params=pltpu.CompilerParams(
            collective_id=0, has_side_effects=True, vmem_limit_bytes=VMEM_LIMIT
        ),
    )(x, gate_w, up_w)


def scatter_kernel(
    ring, gate_grad, up_grad, gate_w, up_w, out_ref, buf, w_buf, w_sem, send_sem, recv_sem
):
    n = len(ring)
    half = buf.shape[3]
    position, right, left = ring_place(ring)

    def load(step, slot):
        copies = []
        for way in range(2):
            shift = 2 * n - 1 - step if way == 0 else 1 + step
            owner = lookup(ring, lax.rem(position + shift, n))
            lines = pl.ds(pl.multiple_of(owner * (2 * half) + way * half, half), half)
            for kind, weight in enumerate((gate_w, up_w)):
                copies.append(
                    pltpu.make_async_copy(
                        weight.at[lines, :], w_buf.at[slot, way, kind], w_sem.at[slot, way, kind]
                    )
                )
        return copies

    for copy in load(0, 0):
        copy.start()
    greet(right, left)

    def hop(step, way):
        return pltpu.make_async_remote_copy(
            src_ref=buf.at[way, step],
            dst_ref=buf.at[way, step + 1],
            send_sem=send_sem.at[way, step],
            recv_sem=recv_sem.at[way, step],
            device_id={"dp": right if way == 0 else left},
            device_id_type=MESH,
        )

    def product(slot, way):
        across = (((1,), (1,)), ((), ()))
        return lax.dot_general(
            gate_grad[...], w_buf[slot, way, 0], across, preferred_element_type=jnp.float32
        ) + lax.dot_general(
            up_grad[...], w_buf[slot, way, 1], across, preferred_element_type=jnp.float32
        )

    def one_step(step, carry):
        slot = lax.rem(step, 2)

        @pl.when(step + 1 < n)
        def _():
            for copy in load(step + 1, lax.rem(step + 1, 2)):
                copy.start()

        for copy in load(step, slot):
            copy.wait()
        for way in range(2):
            part = product(slot, way)

            @pl.when(step == 0)
            def _():
                buf[way, 0] = part.astype(buf.dtype)

            @pl.when(step > 0)
            def _():
                hop(step - 1, way).wait_recv()
                total = buf[way, step].astype(jnp.float32) + part

                @pl.when(step < n - 1)
                def _():
                    buf[way, step] = total.astype(buf.dtype)

                @pl.when(step == n - 1)
                def _():
                    out_ref[way] = total.astype(out_ref.dtype)

            @pl.when(step < n - 1)
            def _():
                hop(step, way).start()

        return carry

    lax.fori_loop(0, n, one_step, 0)

    def finish(step, carry):
        for way in range(2):
            hop(step, way).wait_send()
        return carry

    lax.fori_loop(0, n - 1, finish, 0)


def scatter_rows(ring, gate_grad, up_grad, gate_w, up_w):
    n = len(ring)
    rows, hidden = gate_grad.shape
    half = gate_w.shape[0] // n // 2
    wire = jnp.bfloat16 if n <= SHORT_RING else jnp.float32
    vmem = pl.BlockSpec(memory_space=pltpu.VMEM)
    anywhere = pl.BlockSpec(memory_space=pl.ANY)
    return pl.pallas_call(
        functools.partial(scatter_kernel, ring),
        out_shape=jax.ShapeDtypeStruct((2, rows, half), wire),
        in_specs=[vmem, vmem, anywhere, anywhere],
        out_specs=vmem,
        scratch_shapes=[
            pltpu.VMEM((2, n, rows, half), wire),
            pltpu.VMEM((2, 2, 2, half, hidden), jnp.bfloat16),
            pltpu.SemaphoreType.DMA((2, 2, 2)),
            pltpu.SemaphoreType.DMA((2, n - 1)),
            pltpu.SemaphoreType.DMA((2, n - 1)),
        ],
        compiler_params=pltpu.CompilerParams(
            collective_id=1, has_side_effects=True, vmem_limit_bytes=VMEM_LIMIT
        ),
    )(gate_grad, up_grad, gate_w, up_w)


PAIR = 2
TILE = 256
UP, DOWN, FIRST, LAST, TWIN = range(5)
FRONT_PLAN = (
    ("xl", 0, 0), ("xa", 0, 0), ("xb", 0, 1), ("gl", 0, 1), ("gl", 1, 1), ("xb", 1, 1),
    ("gb", 0, 2), ("gb", 1, 2), ("cx", 0, 2), ("cx", 1, 2), ("cg", 0, 3), ("cg", 1, 3),
)
BACK_LAGS = (2, 3)


def near_first(depth):
    table = []
    for z in range(depth):
        low = 2 * z < depth
        table.append(sorted(range(depth), key=lambda q: (abs(q - z), (q > z) == low)))
    return table


class Seat:
    def __init__(self, depth, far):
        self.depth = depth
        self.dp = lax.axis_index("dp")
        self.expert = lax.axis_index("expert")
        self.z, self.x = lax.div(self.dp, PAIR), lax.rem(self.dp, PAIR)
        self.y, self.core = lax.div(self.expert, PAIR), lax.rem(self.expert, PAIR)
        table = near_first(depth)
        self.table = [q for row in table for q in (row[::-1] if far else row)]
        core, dp, expert = self.core, self.dp, self.expert
        dx, dy = 1 - 2 * self.x, 2 - 4 * self.y
        self.twin = {"dp": dp, "expert": expert + 1 - 2 * core}
        self.across_x = {"dp": dp + dx, "expert": expert}
        self.across_y = {"dp": dp, "expert": expert + dy}
        self.corner = {"dp": dp, "expert": 3 - expert}
        self.first = {"dp": dp + (1 - core) * dx, "expert": expert + core * dy}
        self.last = {"dp": dp + core * dx, "expert": expert + (1 - core) * dy}
        self.up = {"dp": dp + PAIR, "expert": expert}
        self.down = {"dp": dp - PAIR, "expert": expert}
        self.has_up = self.z < depth - 1
        self.has_down = self.z > 0

    def line(self, k):
        return lookup(self.table, self.z * self.depth + k)

    def spot(self, q, a, b):
        core = self.core
        across = lax.rem(self.x + a + core * (b - a), PAIR)
        beside = lax.rem(self.y + b + core * (a - b), PAIR)
        return q * PAIR + across, beside

    def greet(self):
        barrier = pltpu.get_barrier_semaphore()

        def tell(target):
            pl.semaphore_signal(barrier, inc=1, device_id=target, device_id_type=MESH)

        for target in (self.twin, self.across_x, self.across_y, self.corner):
            tell(target)

        @pl.when(self.has_up)
        def _():
            tell(self.up)

        @pl.when(self.has_down)
        def _():
            tell(self.down)

        ends = jnp.where(self.has_up, 1, 0) + jnp.where(self.has_down, 1, 0)
        pl.semaphore_wait(barrier, 4 + ends)


def remote(source, target, send_sem, recv_sem, device):
    return pltpu.make_async_remote_copy(
        src_ref=source, dst_ref=target, send_sem=send_sem, recv_sem=recv_sem,
        device_id=device, device_id_type=MESH,
    )


def run_plan(depth, plan, ops):
    span = depth + max(lag for _, _, lag in plan)

    def turn(i, carry):
        for name, part, lag in plan:

            @pl.when((i >= lag) & (i < lag + depth))
            def _(name=name, part=part, lag=lag):
                ops[name](i - lag, part)

        return carry

    lax.fori_loop(0, span, turn, 0)


def front_kernel(
    depth, main, meta_ref, x_ref, g_ref, gate_w, up_w, down_w, scale_ref, gate_ref, up_ref,
    total_ref, back_ref, full, meta, hot, weight, rows, gate, up, hid, w_buf, d_buf, total,
    own_sem, w_sem, d_sem, note_send, note_recv, send_sem, recv_sem,
):
    seat = Seat(depth, False)
    blocks = PAIR * PAIR
    feat = x_ref.shape[1]
    tok = x_ref.shape[0]
    hidden = gate.shape[1]
    slots = hot.shape[1]
    tile = TILE if hidden % TILE == 0 else hidden
    z = seat.z

    def shard(k, a):
        return seat.line(k) * PAIR + lax.rem(seat.x + a, PAIR)

    def load_up(k, a):
        lines = pl.ds(pl.multiple_of(shard(k, a) * feat, feat), feat)
        return (
            pltpu.make_async_copy(gate_w.at[lines, :], w_buf.at[a, 0], w_sem.at[a, 0]),
            pltpu.make_async_copy(up_w.at[lines, :], w_buf.at[a, 1], w_sem.at[a, 1]),
        )

    def load_down(k, a):
        columns = pl.ds(pl.multiple_of(shard(k, a) * feat, feat), feat)
        return (pltpu.make_async_copy(down_w.at[:, columns], d_buf.at[a], d_sem.at[a]),)

    own = [
        pltpu.make_async_copy(ref, full.at[t, seat.dp, seat.expert], own_sem.at[t])
        for t, ref in enumerate((x_ref, g_ref))
    ]
    for copy in own:
        copy.start()
    meta[seat.expert] = meta_ref[...]
    seat.greet()

    def note(n, target):
        return remote(
            meta_ref, meta.at[seat.expert], note_send.at[n], note_recv.at[seat.expert], target
        )

    notes = [
        note(n, target) for n, target in enumerate((seat.twin, seat.across_y, seat.corner))
    ]

    def link(t, q, a, b, kind):
        d, beside = seat.spot(q, a, b)
        block = beside * PAIR + seat.core
        place = full.at[t, d, block]
        target = (seat.up, seat.down, seat.first, seat.last, seat.twin)[kind]
        number = q * blocks + a * PAIR + b
        return remote(
            place, place, send_sem.at[t, kind, number], recv_sem.at[t, d, block], target
        )

    def arrived(t, q, a, b):
        link(t, q, a, b, TWIN).wait_recv()

    def along(t, q, a, act):
        @pl.when((q <= z) & seat.has_up)
        def _():
            act(link(t, q, a, 0, UP))

        @pl.when((q >= z) & seat.has_down)
        def _():
            act(link(t, q, a, 0, DOWN))

    def begin(copy):
        copy.start()

    def drain(copy):
        copy.wait_send()

    def x_line(k, _):
        q = seat.line(k)

        @pl.when(k > 0)
        def _():
            arrived(0, q, 0, 0)
            along(0, q, 0, begin)
            for kind in (FIRST, LAST, TWIN):
                link(0, q, 0, 0, kind).start()

    def x_first(k, _):
        q = seat.line(k)
        arrived(0, q, 1, 0)
        link(0, q, 1, 0, LAST).start()
        link(0, q, 1, 0, TWIN).start()

    def from_last(t):
        def op(k, a):
            q = seat.line(k)
            arrived(t, q, a, 1)
            link(t, q, a, 1, TWIN).start()

        return op

    def g_line(k, a):
        q = seat.line(k)

        def pass_on():
            arrived(1, q, a, 0)
            along(1, q, a, begin)
            link(1, q, a, 0, LAST).start()
            link(1, q, a, 0, TWIN).start()

        if a:
            pass_on()
        else:
            pl.when(k > 0)(pass_on)

    def dispatch(t, d):
        for beside in range(PAIR):
            block = beside * PAIR + 1 - seat.core
            place = full.at[t, d, block]
            remote(
                place, place, send_sem.at[t, TWIN, 0], recv_sem.at[t, d, block], seat.twin
            ).wait_recv()
        rest = None
        for block in range(blocks):
            got = jnp.dot(hot[block], full[t, d, block], preferred_element_type=jnp.float32)
            if t:
                got = got * weight[block]
            rows[block * main : (block + 1) * main, :] = got[:main].astype(rows.dtype)
            rest = got[main:] if rest is None else rest + got[main:]
        rows[blocks * main :, :] = rest.astype(rows.dtype)

    def again(load, k, a):
        @pl.when(k + 1 < depth)
        def _():
            for copy in load(k + 1, a):
                copy.start()

    def x_products(k, a):
        dispatch(0, shard(k, a))
        for copy in load_up(k, a):
            copy.wait()
        for which, acts in enumerate((gate, up)):
            for n in range(0, hidden, tile):
                columns = slice(n, n + tile)
                acts[:, columns] += jnp.dot(
                    rows[...], w_buf[a, which, :, columns], preferred_element_type=jnp.float32
                )
        again(load_up, k, a)

    def g_products(k, a):
        dispatch(1, shard(k, a))
        for copy in load_down(k, a):
            copy.wait()
        for n in range(0, hidden, tile):
            columns = slice(n, n + tile)
            hid[:, columns] += lax.dot_general(
                rows[...], d_buf[a, columns, :], (((1,), (1,)), ((), ())),
                preferred_element_type=jnp.float32,
            )
        again(load_down, k, a)

    for copy in own:
        copy.wait()
    for copy in notes:
        copy.start()
    along(0, z, 0, begin)
    for kind in (FIRST, LAST, TWIN):
        link(0, z, 0, 0, kind).start()
    along(1, z, 0, begin)
    for kind in (FIRST, LAST, TWIN):
        link(1, z, 0, 0, kind).start()
    for a in range(PAIR):
        for copy in load_up(0, a) + load_down(0, a):
            copy.start()
    for acts in (gate, up, hid, total):
        acts[...] = jnp.zeros_like(acts)

    down_rows = lax.broadcasted_iota(jnp.int32, (tok, tok), 0)
    over_columns = lax.broadcasted_iota(jnp.int32, (tok, tok), 1)
    before = (down_rows < over_columns).astype(jnp.bfloat16)
    slot_rows = lax.broadcasted_iota(jnp.int32, (slots, tok), 0).astype(jnp.float32)
    slot_columns = lax.broadcasted_iota(jnp.int32, (tok, slots), 1).astype(jnp.float32)
    mine = seat.expert.astype(jnp.float32)
    for n, target in enumerate((seat.twin, seat.across_y, seat.corner)):
        other = target["expert"]
        remote(
            meta_ref, meta.at[other], note_send.at[n], note_recv.at[other], target
        ).wait_recv()
    for block in range(blocks):
        notes_in = meta[block]
        named = (notes_in[0:PAIR] == mine).astype(jnp.float32)
        hit = named[0:1] + named[1:PAIR]
        earlier = jnp.dot(
            jnp.broadcast_to(hit, (8, tok)).astype(jnp.bfloat16), before,
            preferred_element_type=jnp.float32,
        )[0:1]
        spilled = jnp.where(earlier < main, earlier, float(main + block))
        want = jnp.where(hit > 0, spilled, -1.0)
        chosen = (slot_rows == want).astype(jnp.float32)
        hot[block] = chosen.astype(hot.dtype)
        share = named[0:1] * notes_in[PAIR : PAIR + 1] + named[1:2] * notes_in[PAIR + 1 : PAIR + 2]
        weight[block] = jnp.sum(chosen * share, axis=1, keepdims=True)
        want_column = jnp.sum(
            jnp.where(down_rows == over_columns, want, 0.0), axis=1, keepdims=True
        )
        back_ref[block] = (slot_columns == want_column).astype(back_ref.dtype)

    run_plan(
        depth, FRONT_PLAN,
        {
            "xl": x_line, "xa": x_first, "xb": from_last(0), "gl": g_line, "gb": from_last(1),
            "cx": x_products, "cg": g_products,
        },
    )

    step = ROW_TILE

    def finish(i, carry):
        lines = pl.ds(pl.multiple_of(i * step, step), step)
        gate_act, up_act, hidden_grad = gate[lines, :], up[lines, :], hid[lines, :]
        sigmoid_gate = jax.nn.sigmoid(gate_act)
        silu_gate = gate_act * sigmoid_gate
        total[...] += hidden_grad * silu_gate * up_act
        scaled_grad = hidden_grad * scale_ref[...]
        up_ref[lines, :] = (scaled_grad * silu_gate).astype(up_ref.dtype)
        gate_ref[lines, :] = (
            scaled_grad * up_act * sigmoid_gate * (1.0 + gate_act * (1.0 - sigmoid_gate))
        ).astype(gate_ref.dtype)
        return carry

    lax.fori_loop(0, gate.shape[0] // step, finish, 0)
    total_ref[...] = jnp.sum(total[...], axis=0, keepdims=True)

    for copy in notes:
        copy.wait_send()

    def settle(k, carry):
        for t in range(2):
            for a in range(PAIR):
                if t or not a:
                    along(t, k, a, drain)
                for b in range(PAIR):
                    link(t, k, a, b, TWIN).wait_send()
                link(t, k, a, 0, LAST).wait_send()
        link(0, k, 0, 0, FIRST).wait_send()
        return carry

    lax.fori_loop(0, depth, settle, 0)
    link(1, z, 0, 0, FIRST).wait_send()


def front(depth, meta, tokens, cotangent, gate_w, up_w, down_w, scale):
    tok, feat = tokens.shape
    hidden = gate_w.shape[1]
    blocks = PAIR * PAIR
    main = 2 * tok // blocks
    slots = main + ROW_TILE
    count = blocks * main + ROW_TILE
    shards = depth * PAIR
    vmem = pl.BlockSpec(memory_space=pltpu.VMEM)
    anywhere = pl.BlockSpec(memory_space=pl.ANY)
    half, wide = jnp.bfloat16, jnp.float32
    dma = pltpu.SemaphoreType.DMA
    return pl.pallas_call(
        functools.partial(front_kernel, depth, main),
        out_shape=(
            jax.ShapeDtypeStruct((count, hidden), half),
            jax.ShapeDtypeStruct((count, hidden), half),
            jax.ShapeDtypeStruct((1, hidden), wide),
            jax.ShapeDtypeStruct((blocks, tok, slots), half),
        ),
        in_specs=[vmem] + [anywhere] * 5 + [vmem],
        out_specs=(vmem, vmem, vmem, vmem),
        scratch_shapes=[
            pltpu.VMEM((2, shards, blocks, tok, feat), half),
            pltpu.VMEM((blocks,) + meta.shape, wide),
            pltpu.VMEM((blocks, slots, tok), half),
            pltpu.VMEM((blocks, slots, 1), wide),
            pltpu.VMEM((count, feat), half),
            pltpu.VMEM((count, hidden), wide),
            pltpu.VMEM((count, hidden), wide),
            pltpu.VMEM((count, hidden), wide),
            pltpu.VMEM((PAIR, 2, feat, hidden), half),
            pltpu.VMEM((PAIR, hidden, feat), half),
            pltpu.VMEM((ROW_TILE, hidden), wide),
            dma((2,)),
            dma((PAIR, 2)),
            dma((PAIR,)),
            dma((3,)),
            dma((blocks,)),
            dma((2, 5, depth * blocks)),
            dma((2, shards, blocks)),
        ],
        compiler_params=pltpu.CompilerParams(
            collective_id=2, has_side_effects=True, vmem_limit_bytes=VMEM_LIMIT
        ),
    )(meta, tokens, cotangent, gate_w, up_w, down_w, scale)


def back_kernel(
    depth, main, gate_grad, up_grad, back, gate_w, up_w, out_ref, prow, kept, away, came, acc,
    out_last, in_last, out_first, in_first, out_line, in_up, in_down, w_buf, w_sem, twin_send,
    twin_recv, last_send, last_recv, first_send, first_recv, line_send, line_recv,
):
    seat = Seat(depth, True)
    blocks = PAIR * PAIR
    tok, feat = out_ref.shape
    shards = depth * PAIR
    tile = TILE if feat % TILE == 0 else feat
    z = seat.z

    def shard(s):
        return seat.line(lax.div(s, PAIR)) * PAIR + lax.rem(seat.x + 1 + s, PAIR)

    def load(s):
        slot = lax.rem(s, 2)
        lines = pl.ds(pl.multiple_of(shard(s) * feat, feat), feat)
        return (
            pltpu.make_async_copy(gate_w.at[lines, :], w_buf.at[slot, 0], w_sem.at[slot, 0]),
            pltpu.make_async_copy(up_w.at[lines, :], w_buf.at[slot, 1], w_sem.at[slot, 1]),
        )

    for copy in load(0):
        copy.start()
    seat.greet()

    def to_twin(d, beside):
        return remote(
            away.at[d, beside], came.at[d, beside], twin_send.at[d, beside],
            twin_recv.at[d, beside], seat.twin,
        )

    def to_last(n):
        return remote(
            out_last.at[n], in_last.at[n], last_send.at[n], last_recv.at[n], seat.last
        )

    def to_first(q):
        return remote(
            out_first.at[q], in_first.at[q], first_send.at[q], first_recv.at[q], seat.first
        )

    def to_up(q):
        return remote(
            out_line.at[q], in_up.at[q], line_send.at[q], line_recv.at[0, q], seat.up
        )

    def to_down(q):
        return remote(
            out_line.at[q], in_down.at[q], line_send.at[q], line_recv.at[1, q], seat.down
        )

    def product(s):
        slot = lax.rem(s, 2)

        @pl.when(s + 1 < shards)
        def _():
            for copy in load(s + 1):
                copy.start()

        for copy in load(s):
            copy.wait()
        across = (((1,), (1,)), ((), ()))
        for n in range(0, feat, tile):
            columns = slice(n, n + tile)
            part = lax.dot_general(
                gate_grad[...], w_buf[slot, 0, columns, :], across,
                preferred_element_type=jnp.float32,
            ) + lax.dot_general(
                up_grad[...], w_buf[slot, 1, columns, :], across,
                preferred_element_type=jnp.float32,
            )
            part = part.astype(prow.dtype)
            for block in range(blocks):
                prow[block, :main, columns] = part[block * main : (block + 1) * main]
                prow[block, main:, columns] = part[blocks * main :]
        d = shard(s)

        def returned(block):
            return jnp.dot(back[block], prow[block], preferred_element_type=jnp.float32)

        for beside in range(PAIR):
            away[d, beside] = returned(beside * PAIR + 1 - seat.core).astype(away.dtype)
            to_twin(d, beside).start()
        for beside in range(PAIR):
            kept[d, beside] = returned(beside * PAIR + seat.core).astype(kept.dtype)

    def products(k, _):
        def one(j, carry):
            product(PAIR * k + j)
            return carry

        lax.fori_loop(0, PAIR, one, 0)

    def wide(ref):
        return ref.astype(jnp.float32)

    def pair_sum(k, _):
        q = seat.line(k)
        for b in (1, 0):
            for a in (1, 0):
                d, beside = seat.spot(q, a, b)
                to_twin(d, beside).wait_recv()
                total = wide(kept[d, beside]) + wide(came[d, beside])
                n = q * PAIR + a
                if b:
                    out_last[n] = total.astype(out_last.dtype)
                    to_last(n).start()
                else:
                    acc[n] = total

    def last_sum(k, _):
        q = seat.line(k)
        for a in (1, 0):
            n = q * PAIR + a
            to_last(n).wait_recv()
            total = acc[n] + wide(in_last[n])
            if a:
                out_first[q] = total.astype(out_first.dtype)
                to_first(q).start()
            else:
                acc[n] = total

    def first_sum(k, _):
        q = seat.line(k)
        n = q * PAIR
        to_first(q).wait_recv()
        acc[n] += wide(in_first[q])

        @pl.when((q >= z) & seat.has_down)
        def _():
            to_up(q).wait_recv()
            acc[n] += wide(in_up[q])

        @pl.when((q <= z) & seat.has_up)
        def _():
            to_down(q).wait_recv()
            acc[n] += wide(in_down[q])

        @pl.when(q != z)
        def _():
            out_line[q] = acc[n].astype(out_line.dtype)

        @pl.when(q > z)
        def _():
            to_up(q).start()

        @pl.when(q < z)
        def _():
            to_down(q).start()

        @pl.when(q == z)
        def _():
            out_ref[...] = acc[n].astype(out_ref.dtype)

    run_plan(
        depth,
        (("mm", 0, 0), ("ps", 0, 0), ("ls", 0, BACK_LAGS[0]), ("fs", 0, BACK_LAGS[1])),
        {"mm": products, "ps": pair_sum, "ls": last_sum, "fs": first_sum},
    )

    def settle(q, carry):
        for j in range(PAIR):
            to_last(q * PAIR + j).wait_send()
            for beside in range(PAIR):
                to_twin(q * PAIR + j, beside).wait_send()
        to_first(q).wait_send()

        @pl.when(q > z)
        def _():
            to_up(q).wait_send()

        @pl.when(q < z)
        def _():
            to_down(q).wait_send()

        return carry

    lax.fori_loop(0, depth, settle, 0)


def back_rows(depth, feat, gate_grad, up_grad, back, gate_w, up_w):
    blocks, tok, slots = back.shape
    count, hidden = gate_grad.shape
    shards = depth * PAIR
    vmem = pl.BlockSpec(memory_space=pltpu.VMEM)
    anywhere = pl.BlockSpec(memory_space=pl.ANY)
    half, wide = jnp.bfloat16, jnp.float32
    dma = pltpu.SemaphoreType.DMA
    piece = (tok, feat)
    return pl.pallas_call(
        functools.partial(back_kernel, depth, slots - ROW_TILE),
        out_shape=jax.ShapeDtypeStruct(piece, half),
        in_specs=[vmem, vmem, vmem, anywhere, anywhere],
        out_specs=vmem,
        scratch_shapes=[
            pltpu.VMEM((blocks, slots, feat), half),
            pltpu.VMEM((shards, PAIR) + piece, half),
            pltpu.VMEM((shards, PAIR) + piece, half),
            pltpu.VMEM((shards, PAIR) + piece, half),
            pltpu.VMEM((shards,) + piece, wide),
            pltpu.VMEM((shards,) + piece, half),
            pltpu.VMEM((shards,) + piece, half),
            pltpu.VMEM((depth,) + piece, half),
            pltpu.VMEM((depth,) + piece, half),
            pltpu.VMEM((depth,) + piece, half),
            pltpu.VMEM((depth,) + piece, half),
            pltpu.VMEM((depth,) + piece, half),
            pltpu.VMEM((2, 2, feat, hidden), half),
            dma((2, 2)),
            dma((shards, PAIR)),
            dma((shards, PAIR)),
            dma((shards,)),
            dma((shards,)),
            dma((depth,)),
            dma((depth,)),
            dma((depth,)),
            dma((2, depth)),
        ],
        compiler_params=pltpu.CompilerParams(
            collective_id=3, has_side_effects=True, vmem_limit_bytes=VMEM_LIMIT
        ),
    )(gate_grad, up_grad, back, gate_w, up_w)


def local_cube(
    depth, tokens, cotangent, expert_ids, combine, w_gate, w_up, w_down, scale_vector
):
    feat = tokens.shape[1]
    meta = jnp.concatenate(
        [expert_ids.astype(jnp.float32).T, combine.T, jnp.zeros((4, tokens.shape[0]))], axis=0
    )
    gate_grad, up_grad, scale_grad, back = front(
        depth, meta, tokens, cotangent, w_gate[0], w_up[0], w_down[0], scale_vector
    )
    token_grads = back_rows(depth, feat, gate_grad, up_grad, back, w_gate[0], w_up[0])
    return token_grads, scale_grad


def local(ring, tokens, cotangent, expert_ids, combine, w_gate, w_up, w_down, scale_vector):
    experts = lax.axis_size("expert")
    tok_count = tokens.shape[0]
    capacity = 2 * tok_count // experts + 1
    dispatch, slot_weight, slot_ids = route_tables(
        expert_ids[None], combine[None], experts, capacity
    )
    dispatch_half = dispatch[0].astype(jnp.bfloat16)
    slot_weight = slot_weight[0]
    flat_index = expert_ids * capacity + slot_ids[0]
    sent_rows = jnp.einsum(
        "ect,td->ecd", dispatch_half, tokens, preferred_element_type=jnp.float32
    ).astype(jnp.bfloat16)
    cot_rows = jnp.einsum(
        "ect,td->ecd", dispatch_half, cotangent, preferred_element_type=jnp.float32
    )
    sent_grads = (slot_weight[:, :, None] * cot_rows).astype(jnp.bfloat16)
    sent = jnp.concatenate([sent_rows, sent_grads], axis=2)
    got = lax.all_to_all(sent, "expert", split_axis=0, concat_axis=0, tiled=True)
    row_count = experts * capacity
    padding = -row_count % ROW_TILE
    x = jnp.pad(got.reshape(row_count, got.shape[2]), ((0, padding), (0, 0)))
    gate_w = w_gate[0]
    up_w = w_up[0]
    down_w = w_down[0]
    gate_act, up_act, grads = gather_acts(ring, x, gate_w, up_w)
    hidden_grad = lax.dot_general(
        grads, down_w, (((1,), (1,)), ((), ())), preferred_element_type=jnp.float32
    )
    sigmoid_gate = jax.nn.sigmoid(gate_act)
    silu_gate = gate_act * sigmoid_gate
    scale_grad = jnp.sum(hidden_grad * silu_gate * up_act, axis=0)
    scaled_grad = hidden_grad * scale_vector[0]
    up_grad = (scaled_grad * silu_gate).astype(jnp.bfloat16)
    gate_grad = (
        scaled_grad * up_act * sigmoid_gate * (1.0 + gate_act * (1.0 - sigmoid_gate))
    ).astype(jnp.bfloat16)
    halves = scatter_rows(ring, gate_grad, up_grad, gate_w, up_w)
    summed = jnp.concatenate([halves[0], halves[1]], axis=1)[:row_count]
    slot_part = summed.reshape(experts, capacity, summed.shape[1])
    returned = lax.all_to_all(slot_part, "expert", split_axis=0, concat_axis=0, tiled=True)
    token_grads = combine_slots(returned.reshape(row_count, returned.shape[2]), flat_index)
    return (token_grads.astype(jnp.bfloat16), scale_grad[None, :])


def solution(mesh):
    placed = (
        P("expert", "dp"),
        P("expert", "dp"),
        P("expert", None),
        P("expert", None),
        P("expert", None, "dp"),
        P("expert", None, "dp"),
        P("expert", "dp", None),
        P("expert", "dp"),
    )
    count = mesh.shape["dp"]
    if mesh.shape["expert"] == PAIR * PAIR and count % PAIR == 0 and count <= SHORT_RING:
        body = functools.partial(local_cube, count // PAIR)
    else:
        body = functools.partial(local, ring_order(mesh))
    return jax.shard_map(
        body,
        mesh=mesh,
        in_specs=placed,
        out_specs=(P("expert", "dp"), P("expert", "dp")),
        check_vma=False,
    )
```

```python
import functools

import jax
import jax.numpy as jnp
from jax import lax
from jax.experimental import pallas as pl
from jax.experimental.pallas import tpu as pltpu
from jax.sharding import PartitionSpec as P


def route_tables(expert_ids, combine, experts, capacity):
    blocks = expert_ids.shape[0]
    per_block = expert_ids.shape[1]
    onehot = (expert_ids[:, :, :, None] == jnp.arange(experts, dtype=jnp.int32)).astype(jnp.int32)
    flat_hits = onehot.reshape(blocks, per_block * 2, experts)
    earlier = jnp.cumsum(flat_hits, axis=1) - flat_hits
    slot_ids = jnp.sum(earlier * flat_hits, axis=2).reshape(blocks, per_block, 2)
    positions = (slot_ids[:, :, :, None] == jnp.arange(capacity, dtype=jnp.int32)).astype(
        jnp.float32
    )
    matches = onehot.astype(jnp.float32)[:, :, :, :, None] * positions[:, :, :, None, :]
    dispatch = jnp.transpose(jnp.sum(matches, axis=2), (0, 2, 3, 1))
    slot_weight = jnp.sum(matches * combine[:, :, :, None, None], axis=(1, 2))
    return (dispatch, slot_weight, slot_ids)


def combine_slots(slot_table, flat_index):
    tok_count = flat_index.shape[0]
    picked = jnp.take(slot_table, flat_index.reshape(-1), axis=0).reshape(
        tok_count, 2, slot_table.shape[1]
    )
    return picked[:, 0].astype(jnp.float32) + picked[:, 1].astype(jnp.float32)


MESH = pl.DeviceIdType.MESH
ROW_TILE = 16
SHORT_RING = 8
VMEM_LIMIT = 60 * 1024 * 1024


def ring_order(mesh):
    count = mesh.shape["dp"]
    devices = mesh.devices.reshape(count, -1)[:, 0]
    places = {}
    for index, device in enumerate(devices):
        coords = getattr(device, "coords", None)
        if coords is None:
            return tuple(range(count))
        places[(coords[2], coords[0])] = index
    zs = sorted({z for z, _ in places})
    xs = sorted({x for _, x in places})
    if len(places) != count or len(zs) * len(xs) != count or len(zs) % 2 or len(xs) < 2:
        return tuple(range(count))
    order = [places[(z, xs[0])] for z in zs]
    for turn, z in enumerate(reversed(zs)):
        order += [places[(z, x)] for x in (xs[1:] if turn % 2 == 0 else xs[:0:-1])]
    return tuple(order)


def lookup(table, key):
    found = jnp.int32(table[0])
    for index in range(1, len(table)):
        found = jnp.where(key == index, jnp.int32(table[index]), found)
    return found


def ring_place(ring):
    n = len(ring)
    position_of = [0] * n
    for position, index in enumerate(ring):
        position_of[index] = position
    position = lookup(position_of, lax.axis_index("dp"))
    right = lookup(ring, lax.rem(position + 1, n))
    left = lookup(ring, lax.rem(position + n - 1, n))
    return position, right, left


def greet(right, left):
    barrier = pltpu.get_barrier_semaphore()
    for neighbour in (left, right):
        pl.semaphore_signal(barrier, inc=1, device_id={"dp": neighbour}, device_id_type=MESH)
    pl.semaphore_wait(barrier, 2)


def gather_kernel(
    ring, tile, x_ref, gate_w, up_w, gate_ref, up_ref, grads_ref, rows_ref, w_buf, w_sem, own_sem,
    send_sem, recv_sem,
):
    n = len(ring)
    width = x_ref.shape[1] // 2
    rows = x_ref.shape[0]
    cut = rows // 2 // ROW_TILE * ROW_TILE
    tiles = gate_w.shape[1] // tile
    position, right, left = ring_place(ring)
    me = lax.axis_index("dp")
    halves = (pl.ds(0, cut), pl.ds(cut, rows - cut))

    def tile_columns(t):
        return pl.ds(0, tile) if tiles == 1 else pl.ds(pl.multiple_of(t * tile, tile), tile)

    def load(t, slot):
        columns = tile_columns(t)
        return (
            pltpu.make_async_copy(gate_w.at[:, columns], w_buf.at[slot, 0], w_sem.at[slot, 0]),
            pltpu.make_async_copy(up_w.at[:, columns], w_buf.at[slot, 1], w_sem.at[slot, 1]),
        )

    for copy in load(0, 0):
        copy.start()

    def columns_of(index):
        return pl.ds(pl.multiple_of(index * width, width), width)

    for which, full in enumerate((rows_ref, grads_ref)):
        own = pltpu.make_async_copy(
            x_ref.at[:, pl.ds(which * width, width)], full.at[:, columns_of(me)], own_sem.at[which]
        )
        own.start()
        own.wait()
    greet(right, left)

    def hop(which, step, way):
        full = (rows_ref, grads_ref)[which]
        shift = n - step if way == 0 else step
        origin = lookup(ring, lax.rem(position + shift, n))
        spot = full.at[halves[way], columns_of(origin)]
        return pltpu.make_async_remote_copy(
            src_ref=spot,
            dst_ref=spot,
            send_sem=send_sem.at[which, way, step],
            recv_sem=recv_sem.at[which, way, step],
            device_id={"dp": right if way == 0 else left},
            device_id_type=MESH,
        )

    def advance(which, step):
        for way in range(2):

            @pl.when(step > 0)
            def _():
                hop(which, step - 1, way).wait_recv()

            hop(which, step, way).start()

    def rows_step(step, carry):
        advance(0, step)
        return carry

    lax.fori_loop(0, n - 1, rows_step, 0)
    for way in range(2):
        hop(1, 0, way).start()
    for way in range(2):
        hop(0, n - 2, way).wait_recv()

    def grads_step(step, carry):
        @pl.when(step > 0)
        def _():
            advance(1, step)

        @pl.when(step < tiles)
        def _():
            slot = lax.rem(step, 2)

            @pl.when(step + 1 < tiles)
            def _():
                for copy in load(step + 1, lax.rem(step + 1, 2)):
                    copy.start()

            columns = tile_columns(step)
            for copy in load(step, slot):
                copy.wait()
            gate_ref[:, columns] = jnp.dot(
                rows_ref[...], w_buf[slot, 0], preferred_element_type=jnp.float32
            )
            up_ref[:, columns] = jnp.dot(
                rows_ref[...], w_buf[slot, 1], preferred_element_type=jnp.float32
            )

        return carry

    lax.fori_loop(0, n - 1, grads_step, 0)
    for way in range(2):
        hop(1, n - 2, way).wait_recv()

    def finish(step, carry):
        for which in range(2):
            for way in range(2):
                hop(which, step, way).wait_send()
        return carry

    lax.fori_loop(0, n - 1, finish, 0)


def gather_acts(ring, x, gate_w, up_w):
    n = len(ring)
    rows, width = x.shape[0], x.shape[1] // 2
    hidden = gate_w.shape[1]
    tile = 256 if hidden % 256 == 0 and hidden // 256 <= n - 1 else hidden
    full = n * width
    vmem = pl.BlockSpec(memory_space=pltpu.VMEM)
    anywhere = pl.BlockSpec(memory_space=pl.ANY)
    return pl.pallas_call(
        functools.partial(gather_kernel, ring, tile),
        out_shape=(
            jax.ShapeDtypeStruct((rows, hidden), jnp.float32),
            jax.ShapeDtypeStruct((rows, hidden), jnp.float32),
            jax.ShapeDtypeStruct((rows, full), jnp.bfloat16),
        ),
        in_specs=[anywhere, anywhere, anywhere],
        out_specs=(vmem, vmem, vmem),
        scratch_shapes=[
            pltpu.VMEM((rows, full), jnp.bfloat16),
            pltpu.VMEM((2, 2, full, tile), jnp.bfloat16),
            pltpu.SemaphoreType.DMA((2, 2)),
            pltpu.SemaphoreType.DMA((2,)),
            pltpu.SemaphoreType.DMA((2, 2, n - 1)),
            pltpu.SemaphoreType.DMA((2, 2, n - 1)),
        ],
        compiler_params=pltpu.CompilerParams(
            collective_id=0, has_side_effects=True, vmem_limit_bytes=VMEM_LIMIT
        ),
    )(x, gate_w, up_w)


def scatter_kernel(
    ring, gate_grad, up_grad, gate_w, up_w, out_ref, buf, w_buf, w_sem, send_sem, recv_sem
):
    n = len(ring)
    half = buf.shape[3]
    position, right, left = ring_place(ring)

    def load(step, slot):
        copies = []
        for way in range(2):
            shift = 2 * n - 1 - step if way == 0 else 1 + step
            owner = lookup(ring, lax.rem(position + shift, n))
            lines = pl.ds(pl.multiple_of(owner * (2 * half) + way * half, half), half)
            for kind, weight in enumerate((gate_w, up_w)):
                copies.append(
                    pltpu.make_async_copy(
                        weight.at[lines, :], w_buf.at[slot, way, kind], w_sem.at[slot, way, kind]
                    )
                )
        return copies

    for copy in load(0, 0):
        copy.start()
    greet(right, left)

    def hop(step, way):
        return pltpu.make_async_remote_copy(
            src_ref=buf.at[way, step],
            dst_ref=buf.at[way, step + 1],
            send_sem=send_sem.at[way, step],
            recv_sem=recv_sem.at[way, step],
            device_id={"dp": right if way == 0 else left},
            device_id_type=MESH,
        )

    def product(slot, way):
        across = (((1,), (1,)), ((), ()))
        return lax.dot_general(
            gate_grad[...], w_buf[slot, way, 0], across, preferred_element_type=jnp.float32
        ) + lax.dot_general(
            up_grad[...], w_buf[slot, way, 1], across, preferred_element_type=jnp.float32
        )

    def one_step(step, carry):
        slot = lax.rem(step, 2)

        @pl.when(step + 1 < n)
        def _():
            for copy in load(step + 1, lax.rem(step + 1, 2)):
                copy.start()

        for copy in load(step, slot):
            copy.wait()
        for way in range(2):
            part = product(slot, way)

            @pl.when(step == 0)
            def _():
                buf[way, 0] = part.astype(buf.dtype)

            @pl.when(step > 0)
            def _():
                hop(step - 1, way).wait_recv()
                total = buf[way, step].astype(jnp.float32) + part

                @pl.when(step < n - 1)
                def _():
                    buf[way, step] = total.astype(buf.dtype)

                @pl.when(step == n - 1)
                def _():
                    out_ref[way] = total.astype(out_ref.dtype)

            @pl.when(step < n - 1)
            def _():
                hop(step, way).start()

        return carry

    lax.fori_loop(0, n, one_step, 0)

    def finish(step, carry):
        for way in range(2):
            hop(step, way).wait_send()
        return carry

    lax.fori_loop(0, n - 1, finish, 0)


def scatter_rows(ring, gate_grad, up_grad, gate_w, up_w):
    n = len(ring)
    rows, hidden = gate_grad.shape
    half = gate_w.shape[0] // n // 2
    wire = jnp.bfloat16 if n <= SHORT_RING else jnp.float32
    vmem = pl.BlockSpec(memory_space=pltpu.VMEM)
    anywhere = pl.BlockSpec(memory_space=pl.ANY)
    return pl.pallas_call(
        functools.partial(scatter_kernel, ring),
        out_shape=jax.ShapeDtypeStruct((2, rows, half), wire),
        in_specs=[vmem, vmem, anywhere, anywhere],
        out_specs=vmem,
        scratch_shapes=[
            pltpu.VMEM((2, n, rows, half), wire),
            pltpu.VMEM((2, 2, 2, half, hidden), jnp.bfloat16),
            pltpu.SemaphoreType.DMA((2, 2, 2)),
            pltpu.SemaphoreType.DMA((2, n - 1)),
            pltpu.SemaphoreType.DMA((2, n - 1)),
        ],
        compiler_params=pltpu.CompilerParams(
            collective_id=1, has_side_effects=True, vmem_limit_bytes=VMEM_LIMIT
        ),
    )(gate_grad, up_grad, gate_w, up_w)


PAIR = 2
TILE = 256
UP, DOWN, FIRST, LAST, TWIN = range(5)
LATE, EARLY = 0, 1
FRONT_PLAN = (
    ("xl", 0, 2),
    ("xb", 1, 4),
    ("cg", 0, 2),
    ("gb", 1, 2),
    ("gl", 1, 1),
    ("cx", 1, 5),
    ("gl", 0, 0),
    ("xb", 0, 3),
    ("cg", 1, 2),
    ("xa", 0, 2),
    ("cx", 0, 3),
    ("gb", 0, 1),
)
BACK_PLAN = (
    ("ps", 0, 1),
    ("fs", 0, 4),
    ("mm", 0, 0),
    ("ps", 1, 2),
    ("mm", 1, 1),
    ("ls", 0, 3),
    ("ls", 1, 2),
)


def near_first(depth):
    table = []
    for z in range(depth):
        low = 2 * z < depth
        table.append(sorted(range(depth), key=lambda q: (abs(q - z), (q > z) == low)))
    return table


class Seat:
    def __init__(self, depth):
        self.depth = depth
        self.dp = lax.axis_index("dp")
        self.expert = lax.axis_index("expert")
        self.z, self.x = lax.div(self.dp, PAIR), lax.rem(self.dp, PAIR)
        self.y, self.core = lax.div(self.expert, PAIR), lax.rem(self.expert, PAIR)
        self.table = [q for row in near_first(depth) for q in row]
        core, dp, expert = self.core, self.dp, self.expert
        dx, dy = 1 - 2 * self.x, 2 - 4 * self.y
        self.twin = {"dp": dp, "expert": expert + 1 - 2 * core}
        self.across_x = {"dp": dp + dx, "expert": expert}
        self.across_y = {"dp": dp, "expert": expert + dy}
        self.corner = {"dp": dp, "expert": 3 - expert}
        self.first = {"dp": dp + (1 - core) * dx, "expert": expert + core * dy}
        self.last = {"dp": dp + core * dx, "expert": expert + (1 - core) * dy}
        self.up = {"dp": dp + PAIR, "expert": expert}
        self.down = {"dp": dp - PAIR, "expert": expert}
        self.has_up = self.z < depth - 1
        self.has_down = self.z > 0

    def line(self, k):
        return lookup(self.table, self.z * self.depth + k)

    def far(self, k):
        return self.line(self.depth - 1 - k)

    def spot(self, q, a, b):
        core = self.core
        across = lax.rem(self.x + a + core * (b - a), PAIR)
        beside = lax.rem(self.y + b + core * (a - b), PAIR)
        return q * PAIR + across, beside

    def greet(self):
        barrier = pltpu.get_barrier_semaphore()

        def tell(target):
            pl.semaphore_signal(barrier, inc=1, device_id=target, device_id_type=MESH)

        for target in (self.twin, self.across_x, self.across_y, self.corner):
            tell(target)

        @pl.when(self.has_up)
        def _():
            tell(self.up)

        @pl.when(self.has_down)
        def _():
            tell(self.down)

        ends = jnp.where(self.has_up, 1, 0) + jnp.where(self.has_down, 1, 0)
        pl.semaphore_wait(barrier, 4 + ends)


def remote(source, target, send_sem, recv_sem, device):
    return pltpu.make_async_remote_copy(
        src_ref=source, dst_ref=target, send_sem=send_sem, recv_sem=recv_sem,
        device_id=device, device_id_type=MESH,
    )


def run_plan(depth, plan, ops):
    span = depth + max(lag for _, _, lag in plan)

    def turn(i, carry):
        for name, part, lag in plan:

            @pl.when((i >= lag) & (i < lag + depth))
            def _(name=name, part=part, lag=lag):
                ops[name](i - lag, part)

        return carry

    lax.fori_loop(0, span, turn, 0)


def cube_kernel(
    depth, main, ids_ref, share_ref, x_ref, g_ref, gate_w, up_w, down_w, scale_ref, out_ref, total_ref,
    full, ids, shares, hot, back, weight, rows, gate, up, hid, w_buf, d_buf, total, gate_grad, up_grad,
    prow, came, acc, in_last, in_first, in_up, in_down, own_sem, w_sem, d_sem, note_send,
    note_recv, send_sem, recv_sem, twin_send, twin_recv, last_send, last_recv, first_send,
    first_recv, line_send, line_recv,
):
    seat = Seat(depth)
    blocks = PAIR * PAIR
    feat = x_ref.shape[1]
    tok = x_ref.shape[0]
    hidden = gate.shape[1]
    slots = hot.shape[1]
    tile = TILE if hidden % TILE == 0 else hidden
    back_tile = TILE if feat % TILE == 0 else feat
    z = seat.z

    def shard(k, a):
        return seat.line(k) * PAIR + lax.rem(seat.x + a, PAIR)

    def load_lines(d, slot):
        lines = pl.ds(pl.multiple_of(d * feat, feat), feat)
        return (
            pltpu.make_async_copy(gate_w.at[lines, :], w_buf.at[slot, 0], w_sem.at[slot, 0]),
            pltpu.make_async_copy(up_w.at[lines, :], w_buf.at[slot, 1], w_sem.at[slot, 1]),
        )

    def load_up(k, a):
        return load_lines(shard(k, a), a)

    def back_shard(k, j):
        return seat.far(k) * PAIR + lax.rem(seat.x + 1 + j, PAIR)

    def load_back(k, j):
        return load_lines(back_shard(k, j), j)

    def load_down(k, a):
        columns = pl.ds(pl.multiple_of(shard(k, a) * feat, feat), feat)
        return (pltpu.make_async_copy(down_w.at[:, columns], d_buf.at[a], d_sem.at[a]),)

    own = [
        pltpu.make_async_copy(ref, full.at[t, seat.dp, seat.expert], own_sem.at[t])
        for t, ref in enumerate((x_ref, g_ref))
    ]
    for copy in own:
        copy.start()
    ids[seat.expert] = ids_ref[...]
    shares[seat.expert] = share_ref[...]
    seat.greet()

    def note(n, ref, table, place, target):
        return remote(
            ref, table.at[seat.expert], note_send.at[n, place], note_recv.at[n, seat.expert], target
        )

    peers = (seat.twin, seat.across_y, seat.corner)
    tables = ((ids_ref, ids), (share_ref, shares))
    notes = [
        note(n, ref, table, place, target)
        for place, target in enumerate(peers)
        for n, (ref, table) in enumerate(tables)
    ]

    def link(t, q, a, b, kind):
        d, beside = seat.spot(q, a, b)
        block = beside * PAIR + seat.core
        place = full.at[t, d, block]
        target = (seat.up, seat.down, seat.first, seat.last, seat.twin)[kind]
        number = q * blocks + a * PAIR + b
        return remote(
            place, place, send_sem.at[t, kind, number], recv_sem.at[t, d, block], target
        )

    def arrived(t, q, a, b):
        link(t, q, a, b, TWIN).wait_recv()

    def along(t, q, a, act):
        @pl.when((q <= z) & seat.has_up)
        def _():
            act(link(t, q, a, 0, UP))

        @pl.when((q >= z) & seat.has_down)
        def _():
            act(link(t, q, a, 0, DOWN))

    def begin(copy):
        copy.start()

    def drain(copy):
        copy.wait_send()

    def early_line(k, _):
        q = seat.line(k)
        pl.when(k > 0)(lambda: arrived(EARLY, q, 0, 0))
        along(EARLY, q, 0, begin)
        for kind in (FIRST, LAST, TWIN):
            link(EARLY, q, 0, 0, kind).start()

    def early_first(k, _):
        q = seat.line(k)
        arrived(EARLY, q, 1, 0)
        link(EARLY, q, 1, 0, LAST).start()
        link(EARLY, q, 1, 0, TWIN).start()

    def from_last(t):
        def op(k, a):
            q = seat.line(k)
            arrived(t, q, a, 1)
            link(t, q, a, 1, TWIN).start()

        return op

    def late_line(k, a):
        q = seat.line(k)

        def pass_on():
            arrived(LATE, q, a, 0)
            along(LATE, q, a, begin)
            link(LATE, q, a, 0, LAST).start()
            link(LATE, q, a, 0, TWIN).start()

        if a:
            pass_on()
        else:
            pl.when(k > 0)(pass_on)

    def dispatch(t, d):
        for beside in range(PAIR):
            block = beside * PAIR + 1 - seat.core
            place = full.at[t, d, block]
            remote(
                place, place, send_sem.at[t, TWIN, 0], recv_sem.at[t, d, block], seat.twin
            ).wait_recv()
        rest = None
        for block in range(blocks):
            got = jnp.dot(hot[block], full[t, d, block], preferred_element_type=jnp.float32)
            if t:
                got = got * weight[block]
            rows[block * main : (block + 1) * main, :] = got[:main].astype(rows.dtype)
            rest = got[main:] if rest is None else rest + got[main:]
        rows[blocks * main :, :] = rest.astype(rows.dtype)

    def again(load, k, a):
        @pl.when(k + 1 < depth)
        def _():
            for copy in load(k + 1, a):
                copy.start()

    def x_products(k, a):
        dispatch(0, shard(k, a))
        for copy in load_up(k, a):
            copy.wait()
        for which, acts in enumerate((gate, up)):
            for n in range(0, hidden, tile):
                columns = slice(n, n + tile)
                acts[:, columns] += jnp.dot(
                    rows[...], w_buf[a, which, :, columns], preferred_element_type=jnp.float32
                )
        again(load_up, k, a)

        @pl.when(k + 1 == depth)
        def _():
            for copy in load_back(0, a):
                copy.start()

    def g_products(k, a):
        dispatch(1, shard(k, a))
        for copy in load_down(k, a):
            copy.wait()
        for n in range(0, hidden, tile):
            columns = slice(n, n + tile)
            hid[:, columns] += lax.dot_general(
                rows[...], d_buf[a, columns, :], (((1,), (1,)), ((), ())),
                preferred_element_type=jnp.float32,
            )
        again(load_down, k, a)

    for copy in own:
        copy.wait()
    for copy in notes:
        copy.start()
    for kind in (FIRST, LAST, TWIN):
        link(LATE, z, 0, 0, kind).start()
    along(LATE, z, 0, begin)
    for a in range(PAIR):
        for copy in load_up(0, a) + load_down(0, a):
            copy.start()
    for acts in (gate, up, hid, total):
        acts[...] = jnp.zeros_like(acts)

    down_rows = lax.broadcasted_iota(jnp.int32, (tok, tok), 0)
    over_columns = lax.broadcasted_iota(jnp.int32, (tok, tok), 1)
    before = (down_rows < over_columns).astype(jnp.bfloat16)
    slot_rows = lax.broadcasted_iota(jnp.int32, (slots, tok), 0).astype(jnp.float32)
    slot_columns = lax.broadcasted_iota(jnp.int32, (tok, slots), 1).astype(jnp.float32)
    same = down_rows == over_columns
    for target in peers:
        other = target["expert"]
        for n, (ref, table) in enumerate(tables):
            remote(
                ref, table.at[other], note_send.at[n, 0], note_recv.at[n, other], target
            ).wait_recv()
    for block in range(blocks):
        named = (ids[block] == seat.expert).astype(jnp.float32)
        hit_column = jnp.sum(named, axis=1, keepdims=True)
        share_column = jnp.sum(named * shares[block], axis=1, keepdims=True)
        hit = jnp.sum(jnp.where(same, hit_column, 0.0), axis=0, keepdims=True)
        share = jnp.sum(jnp.where(same, share_column, 0.0), axis=0, keepdims=True)
        earlier = jnp.dot(
            jnp.broadcast_to(hit, (8, tok)).astype(jnp.bfloat16), before,
            preferred_element_type=jnp.float32,
        )[0:1]
        spilled = jnp.where(earlier < main, earlier, float(main + block))
        want = jnp.where(hit > 0, spilled, -1.0)
        chosen = (slot_rows == want).astype(jnp.float32)
        hot[block] = chosen.astype(hot.dtype)
        weight[block] = jnp.sum(chosen * share, axis=1, keepdims=True)
        want_column = jnp.sum(
            jnp.where(same, want, 0.0), axis=1, keepdims=True
        )
        back[block] = (slot_columns == want_column).astype(back.dtype)

    run_plan(
        depth, FRONT_PLAN,
        {
            "xl": early_line, "xa": early_first, "xb": from_last(EARLY), "gl": late_line,
            "gb": from_last(LATE), "cx": g_products, "cg": x_products,
        },
    )

    step = ROW_TILE

    def finish(i, carry):
        lines = pl.ds(pl.multiple_of(i * step, step), step)
        gate_act, up_act, hidden_grad = gate[lines, :], up[lines, :], hid[lines, :]
        sigmoid_gate = jax.nn.sigmoid(gate_act)
        silu_gate = gate_act * sigmoid_gate
        total[...] += hidden_grad * silu_gate * up_act
        scaled_grad = hidden_grad * scale_ref[...]
        up_grad[lines, :] = (scaled_grad * silu_gate).astype(up_grad.dtype)
        gate_grad[lines, :] = (
            scaled_grad * up_act * sigmoid_gate * (1.0 + gate_act * (1.0 - sigmoid_gate))
        ).astype(gate_grad.dtype)
        return carry

    lax.fori_loop(0, gate.shape[0] // step, finish, 0)
    total_ref[...] = jnp.sum(total[...], axis=0, keepdims=True)

    for copy in notes:
        copy.wait_send()

    def settle(k, carry):
        for t in range(2):
            for a in range(PAIR):
                if t == LATE or not a:
                    along(t, k, a, drain)
                for b in range(PAIR):
                    link(t, k, a, b, TWIN).wait_send()
                link(t, k, a, 0, LAST).wait_send()
        link(EARLY, k, 0, 0, FIRST).wait_send()
        return carry

    lax.fori_loop(0, depth, settle, 0)
    link(LATE, z, 0, 0, FIRST).wait_send()

    def kept(d, beside):
        return full.at[0, d, beside]

    def away(d, beside):
        return full.at[0, d, PAIR + beside]

    def out_last(n):
        return full.at[1, n, 0]

    def out_first(q):
        return full.at[1, q, 1]

    def out_line(q):
        return full.at[1, q, 2]

    def to_twin(d, beside):
        return remote(
            away(d, beside), came.at[d, beside], twin_send.at[d, beside],
            twin_recv.at[d, beside], seat.twin,
        )

    def to_last(n):
        return remote(
            out_last(n), in_last.at[n], last_send.at[n], last_recv.at[n], seat.last
        )

    def to_first(q):
        return remote(
            out_first(q), in_first.at[q], first_send.at[q], first_recv.at[q], seat.first
        )

    def to_up(q):
        return remote(
            out_line(q), in_up.at[q], line_send.at[q], line_recv.at[0, q], seat.up
        )

    def to_down(q):
        return remote(
            out_line(q), in_down.at[q], line_send.at[q], line_recv.at[1, q], seat.down
        )

    def product(k, j):
        for copy in load_back(k, j):
            copy.wait()
        across = (((1,), (1,)), ((), ()))
        for n in range(0, feat, back_tile):
            columns = slice(n, n + back_tile)
            part = lax.dot_general(
                gate_grad[...], w_buf[j, 0, columns, :], across,
                preferred_element_type=jnp.float32,
            ) + lax.dot_general(
                up_grad[...], w_buf[j, 1, columns, :], across,
                preferred_element_type=jnp.float32,
            )
            part = part.astype(prow.dtype)
            for block in range(blocks):
                prow[block, :main, columns] = part[block * main : (block + 1) * main]
                prow[block, main:, columns] = part[blocks * main :]

        @pl.when(k + 1 < depth)
        def _():
            for copy in load_back(k + 1, j):
                copy.start()

        d = back_shard(k, j)

        def returned(block):
            return jnp.dot(back[block], prow[block], preferred_element_type=jnp.float32)

        for beside in range(PAIR):
            away(d, beside)[...] = returned(beside * PAIR + 1 - seat.core).astype(full.dtype)
            to_twin(d, beside).start()
        for beside in range(PAIR):
            kept(d, beside)[...] = returned(beside * PAIR + seat.core).astype(full.dtype)

    def wide(ref):
        return ref.astype(jnp.float32)

    def pair_sum(k, j):
        q = seat.far(k)
        core = seat.core
        for n in (1, 0):
            a = core * n + (1 - core) * (1 - j)
            b = core * (1 - j) + (1 - core) * n
            d, beside = seat.spot(q, a, b)
            to_twin(d, beside).wait_recv()
            total = wide(kept(d, beside)[...]) + wide(came[d, beside])
            m = q * PAIR + a

            @pl.when(b == 1)
            def _(m=m, total=total):
                out_last(m)[...] = total.astype(full.dtype)
                to_last(m).start()

            @pl.when(b == 0)
            def _(m=m, total=total):
                acc[m] = total

    def last_sum(k, a):
        q = seat.far(k)
        n = q * PAIR + a
        to_last(n).wait_recv()
        if a:
            out_first(q)[...] = (acc[n] + wide(in_last[n])).astype(full.dtype)
            to_first(q).start()
        else:
            acc[n] += wide(in_last[n])

    def first_sum(k, _):
        q = seat.far(k)
        n = q * PAIR
        to_first(q).wait_recv()
        acc[n] += wide(in_first[q])

        @pl.when((q >= z) & seat.has_down)
        def _():
            to_up(q).wait_recv()
            acc[n] += wide(in_up[q])

        @pl.when((q <= z) & seat.has_up)
        def _():
            to_down(q).wait_recv()
            acc[n] += wide(in_down[q])

        @pl.when(q != z)
        def _():
            out_line(q)[...] = acc[n].astype(full.dtype)

        @pl.when(q > z)
        def _():
            to_up(q).start()

        @pl.when(q < z)
        def _():
            to_down(q).start()

        @pl.when(q == z)
        def _():
            out_ref[...] = acc[n].astype(out_ref.dtype)

    run_plan(
        depth,
        BACK_PLAN,
        {"mm": product, "ps": pair_sum, "ls": last_sum, "fs": first_sum},
    )

    def settle_back(q, carry):
        for j in range(PAIR):
            to_last(q * PAIR + j).wait_send()
            for beside in range(PAIR):
                to_twin(q * PAIR + j, beside).wait_send()
        to_first(q).wait_send()

        @pl.when(q > z)
        def _():
            to_up(q).wait_send()

        @pl.when(q < z)
        def _():
            to_down(q).wait_send()

        return carry

    lax.fori_loop(0, depth, settle_back, 0)


def cube(depth, expert_ids, combine, tokens, cotangent, gate_w, up_w, down_w, scale):
    tok, feat = tokens.shape
    hidden = gate_w.shape[1]
    blocks = PAIR * PAIR
    main = 2 * tok // blocks
    slots = main + ROW_TILE
    count = blocks * main + ROW_TILE
    shards = depth * PAIR
    vmem = pl.BlockSpec(memory_space=pltpu.VMEM)
    anywhere = pl.BlockSpec(memory_space=pl.ANY)
    half, wide = jnp.bfloat16, jnp.float32
    dma = pltpu.SemaphoreType.DMA
    piece = (tok, feat)
    return pl.pallas_call(
        functools.partial(cube_kernel, depth, main),
        out_shape=(
            jax.ShapeDtypeStruct(piece, half),
            jax.ShapeDtypeStruct((1, hidden), wide),
        ),
        in_specs=[vmem, vmem] + [anywhere] * 5 + [vmem],
        out_specs=(vmem, vmem),
        scratch_shapes=[
            pltpu.VMEM((2, shards, blocks) + piece, half),
            pltpu.VMEM((blocks,) + expert_ids.shape, jnp.int32),
            pltpu.VMEM((blocks,) + combine.shape, wide),
            pltpu.VMEM((blocks, slots, tok), half),
            pltpu.VMEM((blocks, tok, slots), half),
            pltpu.VMEM((blocks, slots, 1), wide),
            pltpu.VMEM((count, feat), half),
            pltpu.VMEM((count, hidden), wide),
            pltpu.VMEM((count, hidden), wide),
            pltpu.VMEM((count, hidden), wide),
            pltpu.VMEM((PAIR, 2, feat, hidden), half),
            pltpu.VMEM((PAIR, hidden, feat), half),
            pltpu.VMEM((ROW_TILE, hidden), wide),
            pltpu.VMEM((count, hidden), half),
            pltpu.VMEM((count, hidden), half),
            pltpu.VMEM((blocks, slots, feat), half),
            pltpu.VMEM((shards, PAIR) + piece, half),
            pltpu.VMEM((shards,) + piece, wide),
            pltpu.VMEM((shards,) + piece, half),
            pltpu.VMEM((depth,) + piece, half),
            pltpu.VMEM((depth,) + piece, half),
            pltpu.VMEM((depth,) + piece, half),
            dma((2,)),
            dma((PAIR, 2)),
            dma((PAIR,)),
            dma((2, 3)),
            dma((2, blocks)),
            dma((2, 5, depth * blocks)),
            dma((2, shards, blocks)),
            dma((shards, PAIR)),
            dma((shards, PAIR)),
            dma((shards,)),
            dma((shards,)),
            dma((depth,)),
            dma((depth,)),
            dma((depth,)),
            dma((2, depth)),
        ],
        compiler_params=pltpu.CompilerParams(
            collective_id=2, has_side_effects=True, vmem_limit_bytes=VMEM_LIMIT
        ),
    )(expert_ids, combine, tokens, cotangent, gate_w, up_w, down_w, scale)


def local_cube(
    depth, tokens, cotangent, expert_ids, combine, w_gate, w_up, w_down, scale_vector
):
    return cube(
        depth, expert_ids, combine, tokens, cotangent, w_gate[0], w_up[0], w_down[0], scale_vector
    )


def local(ring, tokens, cotangent, expert_ids, combine, w_gate, w_up, w_down, scale_vector):
    experts = lax.axis_size("expert")
    tok_count = tokens.shape[0]
    capacity = 2 * tok_count // experts + 1
    dispatch, slot_weight, slot_ids = route_tables(
        expert_ids[None], combine[None], experts, capacity
    )
    dispatch_half = dispatch[0].astype(jnp.bfloat16)
    slot_weight = slot_weight[0]
    flat_index = expert_ids * capacity + slot_ids[0]
    sent_rows = jnp.einsum(
        "ect,td->ecd", dispatch_half, tokens, preferred_element_type=jnp.float32
    ).astype(jnp.bfloat16)
    cot_rows = jnp.einsum(
        "ect,td->ecd", dispatch_half, cotangent, preferred_element_type=jnp.float32
    )
    sent_grads = (slot_weight[:, :, None] * cot_rows).astype(jnp.bfloat16)
    sent = jnp.concatenate([sent_rows, sent_grads], axis=2)
    got = lax.all_to_all(sent, "expert", split_axis=0, concat_axis=0, tiled=True)
    row_count = experts * capacity
    padding = -row_count % ROW_TILE
    x = jnp.pad(got.reshape(row_count, got.shape[2]), ((0, padding), (0, 0)))
    gate_w = w_gate[0]
    up_w = w_up[0]
    down_w = w_down[0]
    gate_act, up_act, grads = gather_acts(ring, x, gate_w, up_w)
    hidden_grad = lax.dot_general(
        grads, down_w, (((1,), (1,)), ((), ())), preferred_element_type=jnp.float32
    )
    sigmoid_gate = jax.nn.sigmoid(gate_act)
    silu_gate = gate_act * sigmoid_gate
    scale_grad = jnp.sum(hidden_grad * silu_gate * up_act, axis=0)
    scaled_grad = hidden_grad * scale_vector[0]
    up_grad = (scaled_grad * silu_gate).astype(jnp.bfloat16)
    gate_grad = (
        scaled_grad * up_act * sigmoid_gate * (1.0 + gate_act * (1.0 - sigmoid_gate))
    ).astype(jnp.bfloat16)
    halves = scatter_rows(ring, gate_grad, up_grad, gate_w, up_w)
    summed = jnp.concatenate([halves[0], halves[1]], axis=1)[:row_count]
    slot_part = summed.reshape(experts, capacity, summed.shape[1])
    returned = lax.all_to_all(slot_part, "expert", split_axis=0, concat_axis=0, tiled=True)
    token_grads = combine_slots(returned.reshape(row_count, returned.shape[2]), flat_index)
    return (token_grads.astype(jnp.bfloat16), scale_grad[None, :])


def solution(mesh):
    placed = (
        P("expert", "dp"),
        P("expert", "dp"),
        P("expert", None),
        P("expert", None),
        P("expert", None, "dp"),
        P("expert", None, "dp"),
        P("expert", "dp", None),
        P("expert", "dp"),
    )
    count = mesh.shape["dp"]
    if mesh.shape["expert"] == PAIR * PAIR and count % PAIR == 0 and count <= SHORT_RING:
        body = functools.partial(local_cube, count // PAIR)
    else:
        body = functools.partial(local, ring_order(mesh))
    return jax.shard_map(
        body,
        mesh=mesh,
        in_specs=placed,
        out_specs=(P("expert", "dp"), P("expert", "dp")),
        check_vma=False,
    )
```

```python
import functools

import jax
import jax.numpy as jnp
from jax import lax
from jax.experimental import pallas as pl
from jax.experimental.pallas import tpu as pltpu
from jax.sharding import PartitionSpec as P


def route_tables(expert_ids, combine, experts, capacity):
    blocks = expert_ids.shape[0]
    per_block = expert_ids.shape[1]
    onehot = (expert_ids[:, :, :, None] == jnp.arange(experts, dtype=jnp.int32)).astype(jnp.int32)
    flat_hits = onehot.reshape(blocks, per_block * 2, experts)
    earlier = jnp.cumsum(flat_hits, axis=1) - flat_hits
    slot_ids = jnp.sum(earlier * flat_hits, axis=2).reshape(blocks, per_block, 2)
    positions = (slot_ids[:, :, :, None] == jnp.arange(capacity, dtype=jnp.int32)).astype(
        jnp.float32
    )
    matches = onehot.astype(jnp.float32)[:, :, :, :, None] * positions[:, :, :, None, :]
    dispatch = jnp.transpose(jnp.sum(matches, axis=2), (0, 2, 3, 1))
    slot_weight = jnp.sum(matches * combine[:, :, :, None, None], axis=(1, 2))
    return (dispatch, slot_weight, slot_ids)


def combine_slots(slot_table, flat_index):
    tok_count = flat_index.shape[0]
    picked = jnp.take(slot_table, flat_index.reshape(-1), axis=0).reshape(
        tok_count, 2, slot_table.shape[1]
    )
    return picked[:, 0].astype(jnp.float32) + picked[:, 1].astype(jnp.float32)


MESH = pl.DeviceIdType.MESH
ROW_TILE = 16
SHORT_RING = 8
VMEM_LIMIT = 60 * 1024 * 1024


def ring_order(mesh):
    count = mesh.shape["dp"]
    devices = mesh.devices.reshape(count, -1)[:, 0]
    places = {}
    for index, device in enumerate(devices):
        coords = getattr(device, "coords", None)
        if coords is None:
            return tuple(range(count))
        places[(coords[2], coords[0])] = index
    zs = sorted({z for z, _ in places})
    xs = sorted({x for _, x in places})
    if len(places) != count or len(zs) * len(xs) != count or len(zs) % 2 or len(xs) < 2:
        return tuple(range(count))
    order = [places[(z, xs[0])] for z in zs]
    for turn, z in enumerate(reversed(zs)):
        order += [places[(z, x)] for x in (xs[1:] if turn % 2 == 0 else xs[:0:-1])]
    return tuple(order)


def lookup(table, key):
    found = jnp.int32(table[0])
    for index in range(1, len(table)):
        found = jnp.where(key == index, jnp.int32(table[index]), found)
    return found


def ring_place(ring):
    n = len(ring)
    position_of = [0] * n
    for position, index in enumerate(ring):
        position_of[index] = position
    position = lookup(position_of, lax.axis_index("dp"))
    right = lookup(ring, lax.rem(position + 1, n))
    left = lookup(ring, lax.rem(position + n - 1, n))
    return position, right, left


def greet(right, left):
    barrier = pltpu.get_barrier_semaphore()
    for neighbour in (left, right):
        pl.semaphore_signal(barrier, inc=1, device_id={"dp": neighbour}, device_id_type=MESH)
    pl.semaphore_wait(barrier, 2)


def gather_kernel(
    ring, tile, x_ref, gate_w, up_w, gate_ref, up_ref, grads_ref, rows_ref, w_buf, w_sem, own_sem,
    send_sem, recv_sem,
):
    n = len(ring)
    width = x_ref.shape[1] // 2
    rows = x_ref.shape[0]
    cut = rows // 2 // ROW_TILE * ROW_TILE
    tiles = gate_w.shape[1] // tile
    position, right, left = ring_place(ring)
    me = lax.axis_index("dp")
    halves = (pl.ds(0, cut), pl.ds(cut, rows - cut))

    def tile_columns(t):
        return pl.ds(0, tile) if tiles == 1 else pl.ds(pl.multiple_of(t * tile, tile), tile)

    def load(t, slot):
        columns = tile_columns(t)
        return (
            pltpu.make_async_copy(gate_w.at[:, columns], w_buf.at[slot, 0], w_sem.at[slot, 0]),
            pltpu.make_async_copy(up_w.at[:, columns], w_buf.at[slot, 1], w_sem.at[slot, 1]),
        )

    for copy in load(0, 0):
        copy.start()

    def columns_of(index):
        return pl.ds(pl.multiple_of(index * width, width), width)

    for which, full in enumerate((rows_ref, grads_ref)):
        own = pltpu.make_async_copy(
            x_ref.at[:, pl.ds(which * width, width)], full.at[:, columns_of(me)], own_sem.at[which]
        )
        own.start()
        own.wait()
    greet(right, left)

    def hop(which, step, way):
        full = (rows_ref, grads_ref)[which]
        shift = n - step if way == 0 else step
        origin = lookup(ring, lax.rem(position + shift, n))
        spot = full.at[halves[way], columns_of(origin)]
        return pltpu.make_async_remote_copy(
            src_ref=spot,
            dst_ref=spot,
            send_sem=send_sem.at[which, way, step],
            recv_sem=recv_sem.at[which, way, step],
            device_id={"dp": right if way == 0 else left},
            device_id_type=MESH,
        )

    def advance(which, step):
        for way in range(2):

            @pl.when(step > 0)
            def _():
                hop(which, step - 1, way).wait_recv()

            hop(which, step, way).start()

    def rows_step(step, carry):
        advance(0, step)
        return carry

    lax.fori_loop(0, n - 1, rows_step, 0)
    for way in range(2):
        hop(1, 0, way).start()
    for way in range(2):
        hop(0, n - 2, way).wait_recv()

    def grads_step(step, carry):
        @pl.when(step > 0)
        def _():
            advance(1, step)

        @pl.when(step < tiles)
        def _():
            slot = lax.rem(step, 2)

            @pl.when(step + 1 < tiles)
            def _():
                for copy in load(step + 1, lax.rem(step + 1, 2)):
                    copy.start()

            columns = tile_columns(step)
            for copy in load(step, slot):
                copy.wait()
            gate_ref[:, columns] = jnp.dot(
                rows_ref[...], w_buf[slot, 0], preferred_element_type=jnp.float32
            )
            up_ref[:, columns] = jnp.dot(
                rows_ref[...], w_buf[slot, 1], preferred_element_type=jnp.float32
            )

        return carry

    lax.fori_loop(0, n - 1, grads_step, 0)
    for way in range(2):
        hop(1, n - 2, way).wait_recv()

    def finish(step, carry):
        for which in range(2):
            for way in range(2):
                hop(which, step, way).wait_send()
        return carry

    lax.fori_loop(0, n - 1, finish, 0)


def gather_acts(ring, x, gate_w, up_w):
    n = len(ring)
    rows, width = x.shape[0], x.shape[1] // 2
    hidden = gate_w.shape[1]
    tile = 256 if hidden % 256 == 0 and hidden // 256 <= n - 1 else hidden
    full = n * width
    vmem = pl.BlockSpec(memory_space=pltpu.VMEM)
    anywhere = pl.BlockSpec(memory_space=pl.ANY)
    return pl.pallas_call(
        functools.partial(gather_kernel, ring, tile),
        out_shape=(
            jax.ShapeDtypeStruct((rows, hidden), jnp.float32),
            jax.ShapeDtypeStruct((rows, hidden), jnp.float32),
            jax.ShapeDtypeStruct((rows, full), jnp.bfloat16),
        ),
        in_specs=[anywhere, anywhere, anywhere],
        out_specs=(vmem, vmem, vmem),
        scratch_shapes=[
            pltpu.VMEM((rows, full), jnp.bfloat16),
            pltpu.VMEM((2, 2, full, tile), jnp.bfloat16),
            pltpu.SemaphoreType.DMA((2, 2)),
            pltpu.SemaphoreType.DMA((2,)),
            pltpu.SemaphoreType.DMA((2, 2, n - 1)),
            pltpu.SemaphoreType.DMA((2, 2, n - 1)),
        ],
        compiler_params=pltpu.CompilerParams(
            collective_id=0, has_side_effects=True, vmem_limit_bytes=VMEM_LIMIT
        ),
    )(x, gate_w, up_w)


def scatter_kernel(
    ring, gate_grad, up_grad, gate_w, up_w, out_ref, buf, w_buf, w_sem, send_sem, recv_sem
):
    n = len(ring)
    half = buf.shape[3]
    position, right, left = ring_place(ring)

    def load(step, slot):
        copies = []
        for way in range(2):
            shift = 2 * n - 1 - step if way == 0 else 1 + step
            owner = lookup(ring, lax.rem(position + shift, n))
            lines = pl.ds(pl.multiple_of(owner * (2 * half) + way * half, half), half)
            for kind, weight in enumerate((gate_w, up_w)):
                copies.append(
                    pltpu.make_async_copy(
                        weight.at[lines, :], w_buf.at[slot, way, kind], w_sem.at[slot, way, kind]
                    )
                )
        return copies

    for copy in load(0, 0):
        copy.start()
    greet(right, left)

    def hop(step, way):
        return pltpu.make_async_remote_copy(
            src_ref=buf.at[way, step],
            dst_ref=buf.at[way, step + 1],
            send_sem=send_sem.at[way, step],
            recv_sem=recv_sem.at[way, step],
            device_id={"dp": right if way == 0 else left},
            device_id_type=MESH,
        )

    def product(slot, way):
        across = (((1,), (1,)), ((), ()))
        return lax.dot_general(
            gate_grad[...], w_buf[slot, way, 0], across, preferred_element_type=jnp.float32
        ) + lax.dot_general(
            up_grad[...], w_buf[slot, way, 1], across, preferred_element_type=jnp.float32
        )

    def one_step(step, carry):
        slot = lax.rem(step, 2)

        @pl.when(step + 1 < n)
        def _():
            for copy in load(step + 1, lax.rem(step + 1, 2)):
                copy.start()

        for copy in load(step, slot):
            copy.wait()
        for way in range(2):
            part = product(slot, way)

            @pl.when(step == 0)
            def _():
                buf[way, 0] = part.astype(buf.dtype)

            @pl.when(step > 0)
            def _():
                hop(step - 1, way).wait_recv()
                total = buf[way, step].astype(jnp.float32) + part

                @pl.when(step < n - 1)
                def _():
                    buf[way, step] = total.astype(buf.dtype)

                @pl.when(step == n - 1)
                def _():
                    out_ref[way] = total.astype(out_ref.dtype)

            @pl.when(step < n - 1)
            def _():
                hop(step, way).start()

        return carry

    lax.fori_loop(0, n, one_step, 0)

    def finish(step, carry):
        for way in range(2):
            hop(step, way).wait_send()
        return carry

    lax.fori_loop(0, n - 1, finish, 0)


def scatter_rows(ring, gate_grad, up_grad, gate_w, up_w):
    n = len(ring)
    rows, hidden = gate_grad.shape
    half = gate_w.shape[0] // n // 2
    wire = jnp.bfloat16 if n <= SHORT_RING else jnp.float32
    vmem = pl.BlockSpec(memory_space=pltpu.VMEM)
    anywhere = pl.BlockSpec(memory_space=pl.ANY)
    return pl.pallas_call(
        functools.partial(scatter_kernel, ring),
        out_shape=jax.ShapeDtypeStruct((2, rows, half), wire),
        in_specs=[vmem, vmem, anywhere, anywhere],
        out_specs=vmem,
        scratch_shapes=[
            pltpu.VMEM((2, n, rows, half), wire),
            pltpu.VMEM((2, 2, 2, half, hidden), jnp.bfloat16),
            pltpu.SemaphoreType.DMA((2, 2, 2)),
            pltpu.SemaphoreType.DMA((2, n - 1)),
            pltpu.SemaphoreType.DMA((2, n - 1)),
        ],
        compiler_params=pltpu.CompilerParams(
            collective_id=1, has_side_effects=True, vmem_limit_bytes=VMEM_LIMIT
        ),
    )(gate_grad, up_grad, gate_w, up_w)


PAIR = 2
TILE = 256
UP, DOWN, FIRST, LAST, TWIN = range(5)
LATE, EARLY = 1, 0
FRONT_PLAN = (
    ("xl", 0, 0), ("gl", 0, 0), ("xl", 1, 0), ("xa", 0, 0), ("xb", 0, 0),
    ("xl", 2, 0), ("gl", 0, 1), ("xb", 1, 0), ("xa", 1, 0), ("cx", 0, 0),
    ("xl", 3, 0), ("gl", 1, 0), ("cx", 1, 0), ("xb", 0, 1), ("gl", 1, 1),
    ("xa", 2, 0), ("cx", 0, 1), ("gl", 2, 0), ("xb", 2, 0), ("gb", 0, 0),
    ("cx", 2, 0), ("xa", 3, 0), ("cg", 0, 0), ("gb", 0, 1), ("gl", 2, 1),
    ("xb", 1, 1), ("cg", 0, 1), ("cx", 1, 1), ("gl", 3, 0), ("gb", 1, 0),
    ("xb", 3, 0), ("cg", 1, 0), ("cx", 3, 0), ("gb", 1, 1), ("gl", 3, 1),
    ("xb", 3, 1), ("xb", 2, 1), ("cg", 1, 1), ("cx", 2, 1), ("gb", 3, 0),
    ("gb", 2, 1), ("gb", 2, 0), ("cg", 2, 0), ("cg", 3, 0), ("gb", 3, 1),
    ("cx", 3, 1), ("cg", 2, 1), ("cg", 3, 1),
)
BACK_PLAN = (
    ("mm", 0, 0), ("mm", 0, 1), ("ps", 0, 0), ("mm", 1, 0), ("ps", 0, 1),
    ("mm", 2, 0), ("ls", 0, 1), ("ps", 1, 0), ("mm", 1, 1), ("mm", 2, 1),
    ("ps", 2, 0), ("ps", 1, 1), ("ls", 0, 0), ("ps", 2, 1), ("fs", 0, 0),
    ("ls", 1, 1), ("mm", 3, 0), ("ls", 2, 1), ("mm", 3, 1), ("ps", 3, 0),
    ("ps", 3, 1), ("ls", 1, 0), ("fs", 1, 0), ("ls", 2, 0), ("fs", 2, 0),
    ("ls", 3, 1), ("ls", 3, 0), ("fs", 3, 0),
)


def near_first(depth):
    table = []
    for z in range(depth):
        low = 2 * z < depth
        table.append(sorted(range(depth), key=lambda q: (abs(q - z), (q > z) == low)))
    return table


class Seat:
    def __init__(self, depth):
        self.depth = depth
        self.dp = lax.axis_index("dp")
        self.expert = lax.axis_index("expert")
        self.z, self.x = lax.div(self.dp, PAIR), lax.rem(self.dp, PAIR)
        self.y, self.core = lax.div(self.expert, PAIR), lax.rem(self.expert, PAIR)
        self.table = [q for row in near_first(depth) for q in row]
        core, dp, expert = self.core, self.dp, self.expert
        dx, dy = 1 - 2 * self.x, 2 - 4 * self.y
        self.twin = {"dp": dp, "expert": expert + 1 - 2 * core}
        self.across_x = {"dp": dp + dx, "expert": expert}
        self.across_y = {"dp": dp, "expert": expert + dy}
        self.corner = {"dp": dp, "expert": 3 - expert}
        self.first = {"dp": dp + (1 - core) * dx, "expert": expert + core * dy}
        self.last = {"dp": dp + core * dx, "expert": expert + (1 - core) * dy}
        self.up = {"dp": dp + PAIR, "expert": expert}
        self.down = {"dp": dp - PAIR, "expert": expert}
        self.has_up = self.z < depth - 1
        self.has_down = self.z > 0

    def line(self, k):
        return lookup(self.table, self.z * self.depth + k)

    def far(self, k):
        return self.line(self.depth - 1 - k)

    def spot(self, q, a, b):
        core = self.core
        across = lax.rem(self.x + a + core * (b - a), PAIR)
        beside = lax.rem(self.y + b + core * (a - b), PAIR)
        return q * PAIR + across, beside

    def greet(self):
        barrier = pltpu.get_barrier_semaphore()

        def tell(target):
            pl.semaphore_signal(barrier, inc=1, device_id=target, device_id_type=MESH)

        for target in (self.twin, self.across_x, self.across_y, self.corner):
            tell(target)

        @pl.when(self.has_up)
        def _():
            tell(self.up)

        @pl.when(self.has_down)
        def _():
            tell(self.down)

        ends = jnp.where(self.has_up, 1, 0) + jnp.where(self.has_down, 1, 0)
        pl.semaphore_wait(barrier, 4 + ends)


def remote(source, target, send_sem, recv_sem, device):
    return pltpu.make_async_remote_copy(
        src_ref=source, dst_ref=target, send_sem=send_sem, recv_sem=recv_sem,
        device_id=device, device_id_type=MESH,
    )


def run_plan(depth, plan, ops):
    names = sorted({(name, part) for name, _, part in plan})
    codes = [names.index((name, part)) * depth + k for name, k, part in plan]

    def turn(i, carry):
        code = lookup(codes, i)
        which, k = lax.div(code, depth), lax.rem(code, depth)
        for index, (name, part) in enumerate(names):

            @pl.when(which == index)
            def _(name=name, part=part):
                ops[name](k, part)

        return carry

    lax.fori_loop(0, len(codes), turn, 0)


def cube_kernel(
    depth, main, ids_ref, share_ref, x_ref, g_ref, gate_w, up_w, down_w, scale_ref, out_ref, total_ref,
    full, memo, memos, hot, back, weight, rows, gate, up, hid, w_buf, d_buf, total, gate_grad, up_grad,
    prow, came, acc, in_last, in_first, in_up, in_down, own_sem, w_sem, d_sem, note_send,
    note_recv, send_sem, recv_sem, twin_send, twin_recv, last_send, last_recv, first_send,
    first_recv, line_send, line_recv,
):
    seat = Seat(depth)
    blocks = PAIR * PAIR
    feat = x_ref.shape[1]
    tok = x_ref.shape[0]
    hidden = gate.shape[1]
    slots = hot.shape[1]
    tile = TILE if hidden % TILE == 0 else hidden
    back_tile = TILE if feat % TILE == 0 else feat
    z = seat.z

    def shard(k, a):
        return seat.line(k) * PAIR + lax.rem(seat.x + a, PAIR)

    def load_lines(d, slot):
        lines = pl.ds(pl.multiple_of(d * feat, feat), feat)
        return (
            pltpu.make_async_copy(gate_w.at[lines, :], w_buf.at[slot, 0], w_sem.at[slot, 0]),
            pltpu.make_async_copy(up_w.at[lines, :], w_buf.at[slot, 1], w_sem.at[slot, 1]),
        )

    def load_up(k, a):
        return load_lines(shard(k, a), a)

    def back_shard(k, j):
        return seat.far(k) * PAIR + lax.rem(seat.x + 1 + j, PAIR)

    def load_back(k, j):
        return load_lines(back_shard(k, j), j)

    def load_down(k, a):
        columns = pl.ds(pl.multiple_of(shard(k, a) * feat, feat), feat)
        return (pltpu.make_async_copy(down_w.at[:, columns], d_buf.at[a], d_sem.at[a]),)

    own = [
        pltpu.make_async_copy(ref, full.at[t, seat.dp, seat.expert], own_sem.at[t])
        for t, ref in enumerate((x_ref, g_ref))
    ]
    for copy in own:
        copy.start()
    down_rows = lax.broadcasted_iota(jnp.int32, (tok, tok), 0)
    over_columns = lax.broadcasted_iota(jnp.int32, (tok, tok), 1)
    same = down_rows == over_columns
    for n, ref in enumerate((ids_ref, share_ref)):
        table = ref[...].astype(jnp.float32)
        for choice in range(PAIR):
            column = table[:, choice : choice + 1]
            row = jnp.sum(jnp.where(same, column, 0.0), axis=0, keepdims=True)
            memo[n * PAIR + choice : n * PAIR + choice + 1, :] = row
    memo[2 * PAIR :, :] = jnp.zeros((memo.shape[0] - 2 * PAIR, tok), jnp.float32)
    memos[seat.expert] = memo[...]
    seat.greet()

    peers = (seat.twin, seat.across_y, seat.corner)

    def note(n, owner):
        return remote(
            memo, memos.at[owner], note_send.at[n], note_recv.at[owner], peers[n]
        )

    notes = [note(n, seat.expert) for n in range(len(peers))]

    def link(t, q, a, b, kind):
        d, beside = seat.spot(q, a, b)
        block = beside * PAIR + seat.core
        place = full.at[t, d, block]
        target = (seat.up, seat.down, seat.first, seat.last, seat.twin)[kind]
        number = q * blocks + a * PAIR + b
        return remote(
            place, place, send_sem.at[t, kind, number], recv_sem.at[t, d, block], target
        )

    def arrived(t, q, a, b):
        link(t, q, a, b, TWIN).wait_recv()

    def along(t, q, a, act):
        @pl.when((q <= z) & seat.has_up)
        def _():
            act(link(t, q, a, 0, UP))

        @pl.when((q >= z) & seat.has_down)
        def _():
            act(link(t, q, a, 0, DOWN))

    def begin(copy):
        copy.start()

    def drain(copy):
        copy.wait_send()

    def early_line(k, _):
        q = seat.line(k)

        @pl.when(k > 0)
        def _():
            arrived(EARLY, q, 0, 0)
            along(EARLY, q, 0, begin)
            for kind in (FIRST, LAST, TWIN):
                link(EARLY, q, 0, 0, kind).start()

    def early_first(k, _):
        q = seat.line(k)
        arrived(EARLY, q, 1, 0)
        link(EARLY, q, 1, 0, LAST).start()
        link(EARLY, q, 1, 0, TWIN).start()

    def from_last(t):
        def op(k, a):
            q = seat.line(k)
            arrived(t, q, a, 1)
            link(t, q, a, 1, TWIN).start()

        return op

    def late_line(k, a):
        q = seat.line(k)

        def pass_on():
            arrived(LATE, q, a, 0)
            along(LATE, q, a, begin)
            link(LATE, q, a, 0, LAST).start()
            link(LATE, q, a, 0, TWIN).start()

        if a:
            pass_on()
        else:
            pl.when(k > 0)(pass_on)

    def dispatch(t, d):
        for beside in range(PAIR):
            block = beside * PAIR + 1 - seat.core
            place = full.at[t, d, block]
            remote(
                place, place, send_sem.at[t, TWIN, 0], recv_sem.at[t, d, block], seat.twin
            ).wait_recv()
        rest = None
        for block in range(blocks):
            got = jnp.dot(hot[block], full[t, d, block], preferred_element_type=jnp.float32)
            if t:
                got = got * weight[block]
            rows[block * main : (block + 1) * main, :] = got[:main].astype(rows.dtype)
            rest = got[main:] if rest is None else rest + got[main:]
        rows[blocks * main :, :] = rest.astype(rows.dtype)

    def again(load, k, a):
        @pl.when(k + 1 < depth)
        def _():
            for copy in load(k + 1, a):
                copy.start()

    def x_products(k, a):
        dispatch(0, shard(k, a))
        for copy in load_up(k, a):
            copy.wait()
        for which, acts in enumerate((gate, up)):
            for n in range(0, hidden, tile):
                columns = slice(n, n + tile)
                acts[:, columns] += jnp.dot(
                    rows[...], w_buf[a, which, :, columns], preferred_element_type=jnp.float32
                )
        again(load_up, k, a)

        @pl.when(k + 1 == depth)
        def _():
            for copy in load_back(0, a):
                copy.start()

    def g_products(k, a):
        dispatch(1, shard(k, a))
        for copy in load_down(k, a):
            copy.wait()
        for n in range(0, hidden, tile):
            columns = slice(n, n + tile)
            hid[:, columns] += lax.dot_general(
                rows[...], d_buf[a, columns, :], (((1,), (1,)), ((), ())),
                preferred_element_type=jnp.float32,
            )
        again(load_down, k, a)

    for copy in own:
        copy.wait()
    for copy in notes:
        copy.start()
    for t in (EARLY, LATE):
        along(t, z, 0, begin)
        for kind in (FIRST, LAST, TWIN):
            link(t, z, 0, 0, kind).start()
    for a in range(PAIR):
        for copy in load_up(0, a) + load_down(0, a):
            copy.start()
    for acts in (gate, up, hid, total):
        acts[...] = jnp.zeros_like(acts)

    before = (down_rows < over_columns).astype(jnp.bfloat16)
    slot_rows = lax.broadcasted_iota(jnp.int32, (slots, tok), 0).astype(jnp.float32)
    slot_columns = lax.broadcasted_iota(jnp.int32, (tok, slots), 1).astype(jnp.float32)
    mine = seat.expert.astype(jnp.float32)
    for n, target in enumerate(peers):
        note(n, target["expert"]).wait_recv()
    for block in range(blocks):
        known = memos[block]
        named = (known[0:PAIR] == mine).astype(jnp.float32)
        hit = named[0:1] + named[1:2]
        share = named[0:1] * known[2:3] + named[1:2] * known[3:4]
        earlier = jnp.dot(
            jnp.broadcast_to(hit, (8, tok)).astype(jnp.bfloat16), before,
            preferred_element_type=jnp.float32,
        )[0:1]
        spilled = jnp.where(earlier < main, earlier, float(main + block))
        want = jnp.where(hit > 0, spilled, -1.0)
        chosen = (slot_rows == want).astype(jnp.float32)
        hot[block] = chosen.astype(hot.dtype)
        weight[block] = jnp.sum(chosen * share, axis=1, keepdims=True)
        want_column = jnp.sum(
            jnp.where(same, want, 0.0), axis=1, keepdims=True
        )
        back[block] = (slot_columns == want_column).astype(back.dtype)

    run_plan(
        depth, FRONT_PLAN,
        {
            "xl": early_line, "xa": early_first, "xb": from_last(EARLY), "gl": late_line,
            "gb": from_last(LATE), "cx": x_products, "cg": g_products,
        },
    )

    step = ROW_TILE

    def finish(i, carry):
        lines = pl.ds(pl.multiple_of(i * step, step), step)
        gate_act, up_act, hidden_grad = gate[lines, :], up[lines, :], hid[lines, :]
        sigmoid_gate = jax.nn.sigmoid(gate_act)
        silu_gate = gate_act * sigmoid_gate
        total[...] += hidden_grad * silu_gate * up_act
        scaled_grad = hidden_grad * scale_ref[...]
        up_grad[lines, :] = (scaled_grad * silu_gate).astype(up_grad.dtype)
        gate_grad[lines, :] = (
            scaled_grad * up_act * sigmoid_gate * (1.0 + gate_act * (1.0 - sigmoid_gate))
        ).astype(gate_grad.dtype)
        return carry

    lax.fori_loop(0, gate.shape[0] // step, finish, 0)
    total_ref[...] = jnp.sum(total[...], axis=0, keepdims=True)

    for copy in notes:
        copy.wait_send()

    def settle(k, carry):
        for t in range(2):
            for a in range(PAIR):
                if t == LATE or not a:
                    along(t, k, a, drain)
                for b in range(PAIR):
                    link(t, k, a, b, TWIN).wait_send()
                link(t, k, a, 0, LAST).wait_send()
        link(EARLY, k, 0, 0, FIRST).wait_send()
        return carry

    lax.fori_loop(0, depth, settle, 0)
    link(LATE, z, 0, 0, FIRST).wait_send()

    def kept(d, beside):
        return full.at[0, d, beside]

    def away(d, beside):
        return full.at[0, d, PAIR + beside]

    def out_last(n):
        return full.at[1, n, 0]

    def out_first(q):
        return full.at[1, q, 1]

    def out_line(q):
        return full.at[1, q, 2]

    def to_twin(d, beside):
        return remote(
            away(d, beside), came.at[d, beside], twin_send.at[d, beside],
            twin_recv.at[d, beside], seat.twin,
        )

    def to_last(n):
        return remote(
            out_last(n), in_last.at[n], last_send.at[n], last_recv.at[n], seat.last
        )

    def to_first(q):
        return remote(
            out_first(q), in_first.at[q], first_send.at[q], first_recv.at[q], seat.first
        )

    def to_up(q):
        return remote(
            out_line(q), in_up.at[q], line_send.at[q], line_recv.at[0, q], seat.up
        )

    def to_down(q):
        return remote(
            out_line(q), in_down.at[q], line_send.at[q], line_recv.at[1, q], seat.down
        )

    def product(k, j):
        for copy in load_back(k, j):
            copy.wait()
        across = (((1,), (1,)), ((), ()))
        for n in range(0, feat, back_tile):
            columns = slice(n, n + back_tile)
            part = lax.dot_general(
                gate_grad[...], w_buf[j, 0, columns, :], across,
                preferred_element_type=jnp.float32,
            ) + lax.dot_general(
                up_grad[...], w_buf[j, 1, columns, :], across,
                preferred_element_type=jnp.float32,
            )
            part = part.astype(prow.dtype)
            for block in range(blocks):
                prow[block, :main, columns] = part[block * main : (block + 1) * main]
                prow[block, main:, columns] = part[blocks * main :]

        @pl.when(k + 1 < depth)
        def _():
            for copy in load_back(k + 1, j):
                copy.start()

        d = back_shard(k, j)

        def returned(block):
            return jnp.dot(back[block], prow[block], preferred_element_type=jnp.float32)

        for beside in range(PAIR):
            away(d, beside)[...] = returned(beside * PAIR + 1 - seat.core).astype(full.dtype)
            to_twin(d, beside).start()
        for beside in range(PAIR):
            kept(d, beside)[...] = returned(beside * PAIR + seat.core).astype(full.dtype)

    def wide(ref):
        return ref.astype(jnp.float32)

    def pair_sum(k, j):
        q = seat.far(k)
        core = seat.core
        for n in (1, 0):
            a = core * n + (1 - core) * (1 - j)
            b = core * (1 - j) + (1 - core) * n
            d, beside = seat.spot(q, a, b)
            to_twin(d, beside).wait_recv()
            total = wide(kept(d, beside)[...]) + wide(came[d, beside])
            m = q * PAIR + a

            @pl.when(b == 1)
            def _(m=m, total=total):
                out_last(m)[...] = total.astype(full.dtype)
                to_last(m).start()

            @pl.when(b == 0)
            def _(m=m, total=total):
                acc[m] = total

    def last_sum(k, a):
        q = seat.far(k)
        n = q * PAIR + a
        to_last(n).wait_recv()
        if a:
            out_first(q)[...] = (acc[n] + wide(in_last[n])).astype(full.dtype)
            to_first(q).start()
        else:
            acc[n] += wide(in_last[n])

    def first_sum(k, _):
        q = seat.far(k)
        n = q * PAIR
        to_first(q).wait_recv()
        acc[n] += wide(in_first[q])

        @pl.when((q >= z) & seat.has_down)
        def _():
            to_up(q).wait_recv()
            acc[n] += wide(in_up[q])

        @pl.when((q <= z) & seat.has_up)
        def _():
            to_down(q).wait_recv()
            acc[n] += wide(in_down[q])

        @pl.when(q != z)
        def _():
            out_line(q)[...] = acc[n].astype(full.dtype)

        @pl.when(q > z)
        def _():
            to_up(q).start()

        @pl.when(q < z)
        def _():
            to_down(q).start()

        @pl.when(q == z)
        def _():
            out_ref[...] = acc[n].astype(out_ref.dtype)

    run_plan(
        depth,
        BACK_PLAN,
        {"mm": product, "ps": pair_sum, "ls": last_sum, "fs": first_sum},
    )

    def settle_back(q, carry):
        for j in range(PAIR):
            to_last(q * PAIR + j).wait_send()
            for beside in range(PAIR):
                to_twin(q * PAIR + j, beside).wait_send()
        to_first(q).wait_send()

        @pl.when(q > z)
        def _():
            to_up(q).wait_send()

        @pl.when(q < z)
        def _():
            to_down(q).wait_send()

        return carry

    lax.fori_loop(0, depth, settle_back, 0)


def cube(depth, expert_ids, combine, tokens, cotangent, gate_w, up_w, down_w, scale):
    tok, feat = tokens.shape
    hidden = gate_w.shape[1]
    blocks = PAIR * PAIR
    main = 2 * tok // blocks
    slots = main + ROW_TILE
    count = blocks * main + ROW_TILE
    shards = depth * PAIR
    vmem = pl.BlockSpec(memory_space=pltpu.VMEM)
    anywhere = pl.BlockSpec(memory_space=pl.ANY)
    half, wide = jnp.bfloat16, jnp.float32
    dma = pltpu.SemaphoreType.DMA
    piece = (tok, feat)
    return pl.pallas_call(
        functools.partial(cube_kernel, depth, main),
        out_shape=(
            jax.ShapeDtypeStruct(piece, half),
            jax.ShapeDtypeStruct((1, hidden), wide),
        ),
        in_specs=[vmem, vmem] + [anywhere] * 5 + [vmem],
        out_specs=(vmem, vmem),
        scratch_shapes=[
            pltpu.VMEM((2, shards, blocks) + piece, half),
            pltpu.VMEM((8, tok), wide),
            pltpu.VMEM((blocks, 8, tok), wide),
            pltpu.VMEM((blocks, slots, tok), half),
            pltpu.VMEM((blocks, tok, slots), half),
            pltpu.VMEM((blocks, slots, 1), wide),
            pltpu.VMEM((count, feat), half),
            pltpu.VMEM((count, hidden), wide),
            pltpu.VMEM((count, hidden), wide),
            pltpu.VMEM((count, hidden), wide),
            pltpu.VMEM((PAIR, 2, feat, hidden), half),
            pltpu.VMEM((PAIR, hidden, feat), half),
            pltpu.VMEM((ROW_TILE, hidden), wide),
            pltpu.VMEM((count, hidden), half),
            pltpu.VMEM((count, hidden), half),
            pltpu.VMEM((blocks, slots, feat), half),
            pltpu.VMEM((shards, PAIR) + piece, half),
            pltpu.VMEM((shards,) + piece, wide),
            pltpu.VMEM((shards,) + piece, half),
            pltpu.VMEM((depth,) + piece, half),
            pltpu.VMEM((depth,) + piece, half),
            pltpu.VMEM((depth,) + piece, half),
            dma((2,)),
            dma((PAIR, 2)),
            dma((PAIR,)),
            dma((3,)),
            dma((blocks,)),
            dma((2, 5, depth * blocks)),
            dma((2, shards, blocks)),
            dma((shards, PAIR)),
            dma((shards, PAIR)),
            dma((shards,)),
            dma((shards,)),
            dma((depth,)),
            dma((depth,)),
            dma((depth,)),
            dma((2, depth)),
        ],
        compiler_params=pltpu.CompilerParams(
            collective_id=2, has_side_effects=True, vmem_limit_bytes=VMEM_LIMIT
        ),
    )(expert_ids, combine, tokens, cotangent, gate_w, up_w, down_w, scale)


def local_cube(
    depth, tokens, cotangent, expert_ids, combine, w_gate, w_up, w_down, scale_vector
):
    return cube(
        depth, expert_ids, combine, tokens, cotangent, w_gate[0], w_up[0], w_down[0], scale_vector
    )


def local(ring, tokens, cotangent, expert_ids, combine, w_gate, w_up, w_down, scale_vector):
    experts = lax.axis_size("expert")
    tok_count = tokens.shape[0]
    capacity = 2 * tok_count // experts + 1
    dispatch, slot_weight, slot_ids = route_tables(
        expert_ids[None], combine[None], experts, capacity
    )
    dispatch_half = dispatch[0].astype(jnp.bfloat16)
    slot_weight = slot_weight[0]
    flat_index = expert_ids * capacity + slot_ids[0]
    sent_rows = jnp.einsum(
        "ect,td->ecd", dispatch_half, tokens, preferred_element_type=jnp.float32
    ).astype(jnp.bfloat16)
    cot_rows = jnp.einsum(
        "ect,td->ecd", dispatch_half, cotangent, preferred_element_type=jnp.float32
    )
    sent_grads = (slot_weight[:, :, None] * cot_rows).astype(jnp.bfloat16)
    sent = jnp.concatenate([sent_rows, sent_grads], axis=2)
    got = lax.all_to_all(sent, "expert", split_axis=0, concat_axis=0, tiled=True)
    row_count = experts * capacity
    padding = -row_count % ROW_TILE
    x = jnp.pad(got.reshape(row_count, got.shape[2]), ((0, padding), (0, 0)))
    gate_w = w_gate[0]
    up_w = w_up[0]
    down_w = w_down[0]
    gate_act, up_act, grads = gather_acts(ring, x, gate_w, up_w)
    hidden_grad = lax.dot_general(
        grads, down_w, (((1,), (1,)), ((), ())), preferred_element_type=jnp.float32
    )
    sigmoid_gate = jax.nn.sigmoid(gate_act)
    silu_gate = gate_act * sigmoid_gate
    scale_grad = jnp.sum(hidden_grad * silu_gate * up_act, axis=0)
    scaled_grad = hidden_grad * scale_vector[0]
    up_grad = (scaled_grad * silu_gate).astype(jnp.bfloat16)
    gate_grad = (
        scaled_grad * up_act * sigmoid_gate * (1.0 + gate_act * (1.0 - sigmoid_gate))
    ).astype(jnp.bfloat16)
    halves = scatter_rows(ring, gate_grad, up_grad, gate_w, up_w)
    summed = jnp.concatenate([halves[0], halves[1]], axis=1)[:row_count]
    slot_part = summed.reshape(experts, capacity, summed.shape[1])
    returned = lax.all_to_all(slot_part, "expert", split_axis=0, concat_axis=0, tiled=True)
    token_grads = combine_slots(returned.reshape(row_count, returned.shape[2]), flat_index)
    return (token_grads.astype(jnp.bfloat16), scale_grad[None, :])


def solution(mesh):
    placed = (
        P("expert", "dp"),
        P("expert", "dp"),
        P("expert", None),
        P("expert", None),
        P("expert", None, "dp"),
        P("expert", None, "dp"),
        P("expert", "dp", None),
        P("expert", "dp"),
    )
    count = mesh.shape["dp"]
    depth = 1 + max(k for _, k, _ in FRONT_PLAN)
    if mesh.shape["expert"] == PAIR * PAIR and count == PAIR * depth:
        body = functools.partial(local_cube, depth)
    else:
        body = functools.partial(local, ring_order(mesh))
    return jax.shard_map(
        body,
        mesh=mesh,
        in_specs=placed,
        out_specs=(P("expert", "dp"), P("expert", "dp")),
        check_vma=False,
    )
```

```python
import functools

import jax
import jax.numpy as jnp
from jax import lax
from jax.experimental import pallas as pl
from jax.experimental.pallas import tpu as pltpu
from jax.sharding import PartitionSpec as P


def route_tables(expert_ids, combine, experts, capacity):
    blocks = expert_ids.shape[0]
    per_block = expert_ids.shape[1]
    onehot = (expert_ids[:, :, :, None] == jnp.arange(experts, dtype=jnp.int32)).astype(jnp.int32)
    flat_hits = onehot.reshape(blocks, per_block * 2, experts)
    earlier = jnp.cumsum(flat_hits, axis=1) - flat_hits
    slot_ids = jnp.sum(earlier * flat_hits, axis=2).reshape(blocks, per_block, 2)
    positions = (slot_ids[:, :, :, None] == jnp.arange(capacity, dtype=jnp.int32)).astype(
        jnp.float32
    )
    matches = onehot.astype(jnp.float32)[:, :, :, :, None] * positions[:, :, :, None, :]
    dispatch = jnp.transpose(jnp.sum(matches, axis=2), (0, 2, 3, 1))
    slot_weight = jnp.sum(matches * combine[:, :, :, None, None], axis=(1, 2))
    return (dispatch, slot_weight, slot_ids)


def combine_slots(slot_table, flat_index):
    tok_count = flat_index.shape[0]
    picked = jnp.take(slot_table, flat_index.reshape(-1), axis=0).reshape(
        tok_count, 2, slot_table.shape[1]
    )
    return picked[:, 0].astype(jnp.float32) + picked[:, 1].astype(jnp.float32)


MESH = pl.DeviceIdType.MESH
ROW_TILE = 16
SHORT_RING = 8
VMEM_LIMIT = 60 * 1024 * 1024


def ring_order(mesh):
    count = mesh.shape["dp"]
    devices = mesh.devices.reshape(count, -1)[:, 0]
    places = {}
    for index, device in enumerate(devices):
        coords = getattr(device, "coords", None)
        if coords is None:
            return tuple(range(count))
        places[(coords[2], coords[0])] = index
    zs = sorted({z for z, _ in places})
    xs = sorted({x for _, x in places})
    if len(places) != count or len(zs) * len(xs) != count or len(zs) % 2 or len(xs) < 2:
        return tuple(range(count))
    order = [places[(z, xs[0])] for z in zs]
    for turn, z in enumerate(reversed(zs)):
        order += [places[(z, x)] for x in (xs[1:] if turn % 2 == 0 else xs[:0:-1])]
    return tuple(order)


def lookup(table, key):
    found = jnp.int32(table[0])
    for index in range(1, len(table)):
        found = jnp.where(key == index, jnp.int32(table[index]), found)
    return found


def ring_place(ring):
    n = len(ring)
    position_of = [0] * n
    for position, index in enumerate(ring):
        position_of[index] = position
    position = lookup(position_of, lax.axis_index("dp"))
    right = lookup(ring, lax.rem(position + 1, n))
    left = lookup(ring, lax.rem(position + n - 1, n))
    return position, right, left


def greet(right, left):
    barrier = pltpu.get_barrier_semaphore()
    for neighbour in (left, right):
        pl.semaphore_signal(barrier, inc=1, device_id={"dp": neighbour}, device_id_type=MESH)
    pl.semaphore_wait(barrier, 2)


def gather_kernel(
    ring, tile, x_ref, gate_w, up_w, gate_ref, up_ref, grads_ref, rows_ref, w_buf, w_sem, own_sem,
    send_sem, recv_sem,
):
    n = len(ring)
    width = x_ref.shape[1] // 2
    rows = x_ref.shape[0]
    cut = rows // 2 // ROW_TILE * ROW_TILE
    tiles = gate_w.shape[1] // tile
    position, right, left = ring_place(ring)
    me = lax.axis_index("dp")
    halves = (pl.ds(0, cut), pl.ds(cut, rows - cut))

    def tile_columns(t):
        return pl.ds(0, tile) if tiles == 1 else pl.ds(pl.multiple_of(t * tile, tile), tile)

    def load(t, slot):
        columns = tile_columns(t)
        return (
            pltpu.make_async_copy(gate_w.at[:, columns], w_buf.at[slot, 0], w_sem.at[slot, 0]),
            pltpu.make_async_copy(up_w.at[:, columns], w_buf.at[slot, 1], w_sem.at[slot, 1]),
        )

    for copy in load(0, 0):
        copy.start()

    def columns_of(index):
        return pl.ds(pl.multiple_of(index * width, width), width)

    for which, full in enumerate((rows_ref, grads_ref)):
        own = pltpu.make_async_copy(
            x_ref.at[:, pl.ds(which * width, width)], full.at[:, columns_of(me)], own_sem.at[which]
        )
        own.start()
        own.wait()
    greet(right, left)

    def hop(which, step, way):
        full = (rows_ref, grads_ref)[which]
        shift = n - step if way == 0 else step
        origin = lookup(ring, lax.rem(position + shift, n))
        spot = full.at[halves[way], columns_of(origin)]
        return pltpu.make_async_remote_copy(
            src_ref=spot,
            dst_ref=spot,
            send_sem=send_sem.at[which, way, step],
            recv_sem=recv_sem.at[which, way, step],
            device_id={"dp": right if way == 0 else left},
            device_id_type=MESH,
        )

    def advance(which, step):
        for way in range(2):

            @pl.when(step > 0)
            def _():
                hop(which, step - 1, way).wait_recv()

            hop(which, step, way).start()

    def rows_step(step, carry):
        advance(0, step)
        return carry

    lax.fori_loop(0, n - 1, rows_step, 0)
    for way in range(2):
        hop(1, 0, way).start()
    for way in range(2):
        hop(0, n - 2, way).wait_recv()

    def grads_step(step, carry):
        @pl.when(step > 0)
        def _():
            advance(1, step)

        @pl.when(step < tiles)
        def _():
            slot = lax.rem(step, 2)

            @pl.when(step + 1 < tiles)
            def _():
                for copy in load(step + 1, lax.rem(step + 1, 2)):
                    copy.start()

            columns = tile_columns(step)
            for copy in load(step, slot):
                copy.wait()
            gate_ref[:, columns] = jnp.dot(
                rows_ref[...], w_buf[slot, 0], preferred_element_type=jnp.float32
            )
            up_ref[:, columns] = jnp.dot(
                rows_ref[...], w_buf[slot, 1], preferred_element_type=jnp.float32
            )

        return carry

    lax.fori_loop(0, n - 1, grads_step, 0)
    for way in range(2):
        hop(1, n - 2, way).wait_recv()

    def finish(step, carry):
        for which in range(2):
            for way in range(2):
                hop(which, step, way).wait_send()
        return carry

    lax.fori_loop(0, n - 1, finish, 0)


def gather_acts(ring, x, gate_w, up_w):
    n = len(ring)
    rows, width = x.shape[0], x.shape[1] // 2
    hidden = gate_w.shape[1]
    tile = 256 if hidden % 256 == 0 and hidden // 256 <= n - 1 else hidden
    full = n * width
    vmem = pl.BlockSpec(memory_space=pltpu.VMEM)
    anywhere = pl.BlockSpec(memory_space=pl.ANY)
    return pl.pallas_call(
        functools.partial(gather_kernel, ring, tile),
        out_shape=(
            jax.ShapeDtypeStruct((rows, hidden), jnp.float32),
            jax.ShapeDtypeStruct((rows, hidden), jnp.float32),
            jax.ShapeDtypeStruct((rows, full), jnp.bfloat16),
        ),
        in_specs=[anywhere, anywhere, anywhere],
        out_specs=(vmem, vmem, vmem),
        scratch_shapes=[
            pltpu.VMEM((rows, full), jnp.bfloat16),
            pltpu.VMEM((2, 2, full, tile), jnp.bfloat16),
            pltpu.SemaphoreType.DMA((2, 2)),
            pltpu.SemaphoreType.DMA((2,)),
            pltpu.SemaphoreType.DMA((2, 2, n - 1)),
            pltpu.SemaphoreType.DMA((2, 2, n - 1)),
        ],
        compiler_params=pltpu.CompilerParams(
            collective_id=0, has_side_effects=True, vmem_limit_bytes=VMEM_LIMIT
        ),
    )(x, gate_w, up_w)


def scatter_kernel(
    ring, gate_grad, up_grad, gate_w, up_w, out_ref, buf, w_buf, w_sem, send_sem, recv_sem
):
    n = len(ring)
    half = buf.shape[3]
    position, right, left = ring_place(ring)

    def load(step, slot):
        copies = []
        for way in range(2):
            shift = 2 * n - 1 - step if way == 0 else 1 + step
            owner = lookup(ring, lax.rem(position + shift, n))
            lines = pl.ds(pl.multiple_of(owner * (2 * half) + way * half, half), half)
            for kind, weight in enumerate((gate_w, up_w)):
                copies.append(
                    pltpu.make_async_copy(
                        weight.at[lines, :], w_buf.at[slot, way, kind], w_sem.at[slot, way, kind]
                    )
                )
        return copies

    for copy in load(0, 0):
        copy.start()
    greet(right, left)

    def hop(step, way):
        return pltpu.make_async_remote_copy(
            src_ref=buf.at[way, step],
            dst_ref=buf.at[way, step + 1],
            send_sem=send_sem.at[way, step],
            recv_sem=recv_sem.at[way, step],
            device_id={"dp": right if way == 0 else left},
            device_id_type=MESH,
        )

    def product(slot, way):
        across = (((1,), (1,)), ((), ()))
        return lax.dot_general(
            gate_grad[...], w_buf[slot, way, 0], across, preferred_element_type=jnp.float32
        ) + lax.dot_general(
            up_grad[...], w_buf[slot, way, 1], across, preferred_element_type=jnp.float32
        )

    def one_step(step, carry):
        slot = lax.rem(step, 2)

        @pl.when(step + 1 < n)
        def _():
            for copy in load(step + 1, lax.rem(step + 1, 2)):
                copy.start()

        for copy in load(step, slot):
            copy.wait()
        for way in range(2):
            part = product(slot, way)

            @pl.when(step == 0)
            def _():
                buf[way, 0] = part.astype(buf.dtype)

            @pl.when(step > 0)
            def _():
                hop(step - 1, way).wait_recv()
                total = buf[way, step].astype(jnp.float32) + part

                @pl.when(step < n - 1)
                def _():
                    buf[way, step] = total.astype(buf.dtype)

                @pl.when(step == n - 1)
                def _():
                    out_ref[way] = total.astype(out_ref.dtype)

            @pl.when(step < n - 1)
            def _():
                hop(step, way).start()

        return carry

    lax.fori_loop(0, n, one_step, 0)

    def finish(step, carry):
        for way in range(2):
            hop(step, way).wait_send()
        return carry

    lax.fori_loop(0, n - 1, finish, 0)


def scatter_rows(ring, gate_grad, up_grad, gate_w, up_w):
    n = len(ring)
    rows, hidden = gate_grad.shape
    half = gate_w.shape[0] // n // 2
    wire = jnp.bfloat16 if n <= SHORT_RING else jnp.float32
    vmem = pl.BlockSpec(memory_space=pltpu.VMEM)
    anywhere = pl.BlockSpec(memory_space=pl.ANY)
    return pl.pallas_call(
        functools.partial(scatter_kernel, ring),
        out_shape=jax.ShapeDtypeStruct((2, rows, half), wire),
        in_specs=[vmem, vmem, anywhere, anywhere],
        out_specs=vmem,
        scratch_shapes=[
            pltpu.VMEM((2, n, rows, half), wire),
            pltpu.VMEM((2, 2, 2, half, hidden), jnp.bfloat16),
            pltpu.SemaphoreType.DMA((2, 2, 2)),
            pltpu.SemaphoreType.DMA((2, n - 1)),
            pltpu.SemaphoreType.DMA((2, n - 1)),
        ],
        compiler_params=pltpu.CompilerParams(
            collective_id=1, has_side_effects=True, vmem_limit_bytes=VMEM_LIMIT
        ),
    )(gate_grad, up_grad, gate_w, up_w)


PAIR = 2
TILE = 256
UP, DOWN, FIRST, LAST, TWIN = range(5)
LATE, EARLY = 1, 0
FRONT_PLAN = (
    ("xl", 0, 0), ("gl", 0, 0), ("xl", 1, 0), ("xa", 0, 0), ("xb", 0, 0),
    ("xl", 2, 0), ("gl", 0, 1), ("xb", 1, 0), ("xa", 1, 0), ("cx", 0, 0),
    ("xl", 3, 0), ("gl", 1, 0), ("cx", 1, 0), ("xb", 0, 1), ("gl", 1, 1),
    ("xa", 2, 0), ("cx", 0, 1), ("gl", 2, 0), ("xb", 2, 0), ("gb", 0, 0),
    ("cx", 2, 0), ("xa", 3, 0), ("cg", 0, 0), ("gb", 0, 1), ("gl", 2, 1),
    ("xb", 1, 1), ("cg", 0, 1), ("cx", 1, 1), ("gl", 3, 0), ("gb", 1, 0),
    ("xb", 3, 0), ("cg", 1, 0), ("cx", 3, 0), ("gb", 1, 1), ("gl", 3, 1),
    ("xb", 3, 1), ("xb", 2, 1), ("cg", 1, 1), ("cx", 2, 1), ("gb", 3, 0),
    ("gb", 2, 1), ("gb", 2, 0), ("cg", 2, 0), ("cg", 3, 0), ("gb", 3, 1),
    ("cx", 3, 1), ("cg", 2, 1), ("cg", 3, 1),
)
BACK_PLAN = (
    ("mm", 0, 0), ("mm", 0, 1), ("ps", 0, 0), ("mm", 1, 0), ("ps", 0, 1),
    ("mm", 2, 0), ("ls", 0, 1), ("ps", 1, 0), ("mm", 1, 1), ("mm", 2, 1),
    ("ps", 2, 0), ("ps", 1, 1), ("ls", 0, 0), ("ps", 2, 1), ("fs", 0, 0),
    ("ls", 1, 1), ("mm", 3, 0), ("ls", 2, 1), ("mm", 3, 1), ("ps", 3, 0),
    ("ps", 3, 1), ("ls", 1, 0), ("fs", 1, 0), ("ls", 2, 0), ("fs", 2, 0),
    ("ls", 3, 1), ("ls", 3, 0), ("fs", 3, 0),
)


def near_first(depth):
    table = []
    for z in range(depth):
        low = 2 * z < depth
        table.append(sorted(range(depth), key=lambda q: (abs(q - z), (q > z) == low)))
    return table


class Seat:
    def __init__(self, depth):
        self.depth = depth
        self.dp = lax.axis_index("dp")
        self.expert = lax.axis_index("expert")
        self.z, self.x = lax.div(self.dp, PAIR), lax.rem(self.dp, PAIR)
        self.y, self.core = lax.div(self.expert, PAIR), lax.rem(self.expert, PAIR)
        self.order = [
            lookup([row[k] for row in near_first(depth)], self.z) for k in range(depth)
        ]
        core, dp, expert = self.core, self.dp, self.expert
        dx, dy = 1 - 2 * self.x, 2 - 4 * self.y
        self.twin = {"dp": dp, "expert": expert + 1 - 2 * core}
        self.across_x = {"dp": dp + dx, "expert": expert}
        self.across_y = {"dp": dp, "expert": expert + dy}
        self.corner = {"dp": dp, "expert": 3 - expert}
        self.first = {"dp": dp + (1 - core) * dx, "expert": expert + core * dy}
        self.last = {"dp": dp + core * dx, "expert": expert + (1 - core) * dy}
        self.up = {"dp": dp + PAIR, "expert": expert}
        self.down = {"dp": dp - PAIR, "expert": expert}
        self.has_up = self.z < depth - 1
        self.has_down = self.z > 0

    def line(self, k):
        found = self.order[0]
        for index in range(1, self.depth):
            found = jnp.where(k == index, self.order[index], found)
        return found

    def far(self, k):
        return self.line(self.depth - 1 - k)

    def spot(self, q, a, b):
        core = self.core
        across = lax.rem(self.x + a + core * (b - a), PAIR)
        beside = lax.rem(self.y + b + core * (a - b), PAIR)
        return q * PAIR + across, beside

    def greet(self):
        barrier = pltpu.get_barrier_semaphore()

        def tell(target):
            pl.semaphore_signal(barrier, inc=1, device_id=target, device_id_type=MESH)

        for target in (self.twin, self.across_x, self.across_y, self.corner):
            tell(target)

        @pl.when(self.has_up)
        def _():
            tell(self.up)

        @pl.when(self.has_down)
        def _():
            tell(self.down)

        ends = jnp.where(self.has_up, 1, 0) + jnp.where(self.has_down, 1, 0)
        pl.semaphore_wait(barrier, 4 + ends)


def remote(source, target, send_sem, recv_sem, device):
    return pltpu.make_async_remote_copy(
        src_ref=source, dst_ref=target, send_sem=send_sem, recv_sem=recv_sem,
        device_id=device, device_id_type=MESH,
    )


def run_plan(depth, plan, ops):
    names = sorted({(name, part) for name, _, part in plan})
    codes = [names.index((name, part)) * depth + k for name, k, part in plan]
    base = 1 << (len(names) * depth - 1).bit_length()
    group = 1
    while base ** (group + 1) < 2**31 and group < 4:
        group += 1
    while len(codes) % group:
        group -= 1
    words = [
        sum(code * base**n for n, code in enumerate(codes[i : i + group]))
        for i in range(0, len(codes), group)
    ]

    def pick(which, k, low, high):
        if high - low == 1:
            name, part = names[low]
            ops[name](k, part)
            return
        middle = (low + high) // 2
        lax.cond(
            which < middle,
            lambda: pick(which, k, low, middle),
            lambda: pick(which, k, middle, high),
        )

    def turn(i, carry):
        def one(_, word):
            code = lax.rem(word, base)
            pick(lax.div(code, depth), lax.rem(code, depth), 0, len(names))
            return lax.div(word, base)

        lax.fori_loop(0, group, one, lookup(words, i))
        return carry

    lax.fori_loop(0, len(words), turn, 0)


def cube_kernel(
    depth, main, ids_ref, share_ref, x_ref, g_ref, gate_w, up_w, down_w, scale_ref, out_ref, total_ref,
    full, memo, memos, hot, back, weight, rows, gate, up, hid, w_buf, d_buf, total, gate_grad, up_grad,
    prow, came, acc, in_last, in_first, in_up, in_down, own_sem, w_sem, d_sem, note_send,
    note_recv, send_sem, recv_sem, twin_send, twin_recv, last_send, last_recv, first_send,
    first_recv, line_send, line_recv,
):
    seat = Seat(depth)
    blocks = PAIR * PAIR
    feat = x_ref.shape[1]
    tok = x_ref.shape[0]
    hidden = gate.shape[1]
    slots = hot.shape[1]
    tile = TILE if hidden % TILE == 0 else hidden
    back_tile = TILE if feat % TILE == 0 else feat
    z = seat.z

    def shard(k, a):
        return seat.line(k) * PAIR + lax.rem(seat.x + a, PAIR)

    def load_lines(d, slot):
        lines = pl.ds(pl.multiple_of(d * feat, feat), feat)
        return (
            pltpu.make_async_copy(gate_w.at[lines, :], w_buf.at[slot, 0], w_sem.at[slot, 0]),
            pltpu.make_async_copy(up_w.at[lines, :], w_buf.at[slot, 1], w_sem.at[slot, 1]),
        )

    def load_up(k, a):
        return load_lines(shard(k, a), a)

    def back_shard(k, j):
        return seat.far(k) * PAIR + lax.rem(seat.x + 1 + j, PAIR)

    def load_back(k, j):
        return load_lines(back_shard(k, j), j)

    def load_down(k, a):
        columns = pl.ds(pl.multiple_of(shard(k, a) * feat, feat), feat)
        return (pltpu.make_async_copy(down_w.at[:, columns], d_buf.at[a], d_sem.at[a]),)

    own = [
        pltpu.make_async_copy(ref, full.at[t, seat.dp, seat.expert], own_sem.at[t])
        for t, ref in enumerate((x_ref, g_ref))
    ]
    for copy in own:
        copy.start()
    down_rows = lax.broadcasted_iota(jnp.int32, (tok, tok), 0)
    over_columns = lax.broadcasted_iota(jnp.int32, (tok, tok), 1)
    same = down_rows == over_columns
    for n, ref in enumerate((ids_ref, share_ref)):
        table = ref[...].astype(jnp.float32)
        for choice in range(PAIR):
            column = table[:, choice : choice + 1]
            row = jnp.sum(jnp.where(same, column, 0.0), axis=0, keepdims=True)
            memo[n * PAIR + choice : n * PAIR + choice + 1, :] = row
    memo[2 * PAIR :, :] = jnp.zeros((memo.shape[0] - 2 * PAIR, tok), jnp.float32)
    memos[seat.expert] = memo[...]
    seat.greet()

    peers = (seat.twin, seat.across_y, seat.corner)

    def note(n, owner):
        return remote(
            memo, memos.at[owner], note_send.at[n], note_recv.at[owner], peers[n]
        )

    notes = [note(n, seat.expert) for n in range(len(peers))]

    def link(t, q, a, b, kind):
        d, beside = seat.spot(q, a, b)
        block = beside * PAIR + seat.core
        place = full.at[t, d, block]
        target = (seat.up, seat.down, seat.first, seat.last, seat.twin)[kind]
        number = q * blocks + a * PAIR + b
        return remote(
            place, place, send_sem.at[t, kind, number], recv_sem.at[t, d, block], target
        )

    def arrived(t, q, a, b):
        link(t, q, a, b, TWIN).wait_recv()

    def along(t, q, a, act):
        @pl.when((q <= z) & seat.has_up)
        def _():
            act(link(t, q, a, 0, UP))

        @pl.when((q >= z) & seat.has_down)
        def _():
            act(link(t, q, a, 0, DOWN))

    def begin(copy):
        copy.start()

    def drain(copy):
        copy.wait_send()

    def early_line(k, _):
        q = seat.line(k)

        @pl.when(k > 0)
        def _():
            arrived(EARLY, q, 0, 0)
            along(EARLY, q, 0, begin)
            for kind in (FIRST, LAST, TWIN):
                link(EARLY, q, 0, 0, kind).start()

    def early_first(k, _):
        q = seat.line(k)
        arrived(EARLY, q, 1, 0)
        link(EARLY, q, 1, 0, LAST).start()
        link(EARLY, q, 1, 0, TWIN).start()

    def from_last(t):
        def op(k, a):
            q = seat.line(k)
            arrived(t, q, a, 1)
            link(t, q, a, 1, TWIN).start()

        return op

    def late_line(k, a):
        q = seat.line(k)

        def pass_on():
            arrived(LATE, q, a, 0)
            along(LATE, q, a, begin)
            link(LATE, q, a, 0, LAST).start()
            link(LATE, q, a, 0, TWIN).start()

        if a:
            pass_on()
        else:
            pl.when(k > 0)(pass_on)

    def dispatch(t, d):
        for beside in range(PAIR):
            block = beside * PAIR + 1 - seat.core
            place = full.at[t, d, block]
            remote(
                place, place, send_sem.at[t, TWIN, 0], recv_sem.at[t, d, block], seat.twin
            ).wait_recv()
        rest = None
        for block in range(blocks):
            got = jnp.dot(hot[block], full[t, d, block], preferred_element_type=jnp.float32)
            if t:
                got = got * weight[block]
            rows[block * main : (block + 1) * main, :] = got[:main].astype(rows.dtype)
            rest = got[main:] if rest is None else rest + got[main:]
        rows[blocks * main :, :] = rest.astype(rows.dtype)

    def again(load, k, a):
        @pl.when(k + 1 < depth)
        def _():
            for copy in load(k + 1, a):
                copy.start()

    def x_products(k, a):
        dispatch(0, shard(k, a))
        for copy in load_up(k, a):
            copy.wait()
        for which, acts in enumerate((gate, up)):
            for n in range(0, hidden, tile):
                columns = slice(n, n + tile)
                acts[:, columns] += jnp.dot(
                    rows[...], w_buf[a, which, :, columns], preferred_element_type=jnp.float32
                )
        again(load_up, k, a)

        @pl.when(k + 1 == depth)
        def _():
            for copy in load_back(0, a):
                copy.start()

    def g_products(k, a):
        dispatch(1, shard(k, a))
        for copy in load_down(k, a):
            copy.wait()
        for n in range(0, hidden, tile):
            columns = slice(n, n + tile)
            hid[:, columns] += lax.dot_general(
                rows[...], d_buf[a, columns, :], (((1,), (1,)), ((), ())),
                preferred_element_type=jnp.float32,
            )
        again(load_down, k, a)

    for copy in own:
        copy.wait()
    for copy in notes:
        copy.start()
    for t in (EARLY, LATE):
        along(t, z, 0, begin)
        for kind in (FIRST, LAST, TWIN):
            link(t, z, 0, 0, kind).start()
    for a in range(PAIR):
        for copy in load_up(0, a) + load_down(0, a):
            copy.start()
    for acts in (gate, up, hid, total):
        acts[...] = jnp.zeros_like(acts)

    before = (down_rows < over_columns).astype(jnp.bfloat16)
    slot_rows = lax.broadcasted_iota(jnp.int32, (slots, tok), 0).astype(jnp.float32)
    slot_columns = lax.broadcasted_iota(jnp.int32, (tok, slots), 1).astype(jnp.float32)
    mine = seat.expert.astype(jnp.float32)
    for n, target in enumerate(peers):
        note(n, target["expert"]).wait_recv()
    for block in range(blocks):
        known = memos[block]
        named = (known[0:PAIR] == mine).astype(jnp.float32)
        hit = named[0:1] + named[1:2]
        share = named[0:1] * known[2:3] + named[1:2] * known[3:4]
        earlier = jnp.dot(
            jnp.broadcast_to(hit, (8, tok)).astype(jnp.bfloat16), before,
            preferred_element_type=jnp.float32,
        )[0:1]
        spilled = jnp.where(earlier < main, earlier, float(main + block))
        want = jnp.where(hit > 0, spilled, -1.0)
        chosen = (slot_rows == want).astype(jnp.float32)
        hot[block] = chosen.astype(hot.dtype)
        weight[block] = jnp.sum(chosen * share, axis=1, keepdims=True)
        want_column = jnp.sum(
            jnp.where(same, want, 0.0), axis=1, keepdims=True
        )
        back[block] = (slot_columns == want_column).astype(back.dtype)

    run_plan(
        depth, FRONT_PLAN,
        {
            "xl": early_line, "xa": early_first, "xb": from_last(EARLY), "gl": late_line,
            "gb": from_last(LATE), "cx": x_products, "cg": g_products,
        },
    )

    step = ROW_TILE

    def finish(i, carry):
        lines = pl.ds(pl.multiple_of(i * step, step), step)
        gate_act, up_act, hidden_grad = gate[lines, :], up[lines, :], hid[lines, :]
        sigmoid_gate = jax.nn.sigmoid(gate_act)
        silu_gate = gate_act * sigmoid_gate
        total[...] += hidden_grad * silu_gate * up_act
        scaled_grad = hidden_grad * scale_ref[...]
        up_grad[lines, :] = (scaled_grad * silu_gate).astype(up_grad.dtype)
        gate_grad[lines, :] = (
            scaled_grad * up_act * sigmoid_gate * (1.0 + gate_act * (1.0 - sigmoid_gate))
        ).astype(gate_grad.dtype)
        return carry

    lax.fori_loop(0, gate.shape[0] // step, finish, 0)
    total_ref[...] = jnp.sum(total[...], axis=0, keepdims=True)

    for copy in notes:
        copy.wait_send()

    def settle(k, carry):
        for t in range(2):
            for a in range(PAIR):
                if t == LATE or not a:
                    along(t, k, a, drain)
                for b in range(PAIR):
                    link(t, k, a, b, TWIN).wait_send()
                link(t, k, a, 0, LAST).wait_send()
        link(EARLY, k, 0, 0, FIRST).wait_send()
        return carry

    lax.fori_loop(0, depth, settle, 0)
    link(LATE, z, 0, 0, FIRST).wait_send()

    def kept(d, beside):
        return full.at[0, d, beside]

    def away(d, beside):
        return full.at[0, d, PAIR + beside]

    def out_last(n):
        return full.at[1, n, 0]

    def out_first(q):
        return full.at[1, q, 1]

    def out_line(q):
        return full.at[1, q, 2]

    def to_twin(d, beside):
        return remote(
            away(d, beside), came.at[d, beside], twin_send.at[d, beside],
            twin_recv.at[d, beside], seat.twin,
        )

    def to_last(n):
        return remote(
            out_last(n), in_last.at[n], last_send.at[n], last_recv.at[n], seat.last
        )

    def to_first(q):
        return remote(
            out_first(q), in_first.at[q], first_send.at[q], first_recv.at[q], seat.first
        )

    def to_up(q):
        return remote(
            out_line(q), in_up.at[q], line_send.at[q], line_recv.at[0, q], seat.up
        )

    def to_down(q):
        return remote(
            out_line(q), in_down.at[q], line_send.at[q], line_recv.at[1, q], seat.down
        )

    def product(k, j):
        for copy in load_back(k, j):
            copy.wait()
        across = (((1,), (1,)), ((), ()))
        for n in range(0, feat, back_tile):
            columns = slice(n, n + back_tile)
            part = lax.dot_general(
                gate_grad[...], w_buf[j, 0, columns, :], across,
                preferred_element_type=jnp.float32,
            ) + lax.dot_general(
                up_grad[...], w_buf[j, 1, columns, :], across,
                preferred_element_type=jnp.float32,
            )
            part = part.astype(prow.dtype)
            for block in range(blocks):
                prow[block, :main, columns] = part[block * main : (block + 1) * main]
                prow[block, main:, columns] = part[blocks * main :]

        @pl.when(k + 1 < depth)
        def _():
            for copy in load_back(k + 1, j):
                copy.start()

        d = back_shard(k, j)

        def returned(block):
            return jnp.dot(back[block], prow[block], preferred_element_type=jnp.float32)

        for beside in range(PAIR):
            away(d, beside)[...] = returned(beside * PAIR + 1 - seat.core).astype(full.dtype)
            to_twin(d, beside).start()
        for beside in range(PAIR):
            kept(d, beside)[...] = returned(beside * PAIR + seat.core).astype(full.dtype)

    def wide(ref):
        return ref.astype(jnp.float32)

    def pair_sum(k, j):
        q = seat.far(k)
        core = seat.core
        for n in (1, 0):
            a = core * n + (1 - core) * (1 - j)
            b = core * (1 - j) + (1 - core) * n
            d, beside = seat.spot(q, a, b)
            to_twin(d, beside).wait_recv()
            total = wide(kept(d, beside)[...]) + wide(came[d, beside])
            m = q * PAIR + a

            @pl.when(b == 1)
            def _(m=m, total=total):
                out_last(m)[...] = total.astype(full.dtype)
                to_last(m).start()

            @pl.when(b == 0)
            def _(m=m, total=total):
                acc[m] = total

    def last_sum(k, a):
        q = seat.far(k)
        n = q * PAIR + a
        to_last(n).wait_recv()
        if a:
            out_first(q)[...] = (acc[n] + wide(in_last[n])).astype(full.dtype)
            to_first(q).start()
        else:
            acc[n] += wide(in_last[n])

    def first_sum(k, _):
        q = seat.far(k)
        n = q * PAIR
        to_first(q).wait_recv()
        acc[n] += wide(in_first[q])

        @pl.when((q >= z) & seat.has_down)
        def _():
            to_up(q).wait_recv()
            acc[n] += wide(in_up[q])

        @pl.when((q <= z) & seat.has_up)
        def _():
            to_down(q).wait_recv()
            acc[n] += wide(in_down[q])

        @pl.when(q != z)
        def _():
            out_line(q)[...] = acc[n].astype(full.dtype)

        @pl.when(q > z)
        def _():
            to_up(q).start()

        @pl.when(q < z)
        def _():
            to_down(q).start()

        @pl.when(q == z)
        def _():
            out_ref[...] = acc[n].astype(out_ref.dtype)

    run_plan(
        depth,
        BACK_PLAN,
        {"mm": product, "ps": pair_sum, "ls": last_sum, "fs": first_sum},
    )

    def settle_back(q, carry):
        for j in range(PAIR):
            to_last(q * PAIR + j).wait_send()
            for beside in range(PAIR):
                to_twin(q * PAIR + j, beside).wait_send()
        to_first(q).wait_send()

        @pl.when(q > z)
        def _():
            to_up(q).wait_send()

        @pl.when(q < z)
        def _():
            to_down(q).wait_send()

        return carry

    lax.fori_loop(0, depth, settle_back, 0)


def cube(depth, expert_ids, combine, tokens, cotangent, gate_w, up_w, down_w, scale):
    tok, feat = tokens.shape
    hidden = gate_w.shape[1]
    blocks = PAIR * PAIR
    main = 2 * tok // blocks
    slots = main + ROW_TILE
    count = blocks * main + ROW_TILE
    shards = depth * PAIR
    vmem = pl.BlockSpec(memory_space=pltpu.VMEM)
    anywhere = pl.BlockSpec(memory_space=pl.ANY)
    half, wide = jnp.bfloat16, jnp.float32
    dma = pltpu.SemaphoreType.DMA
    piece = (tok, feat)
    return pl.pallas_call(
        functools.partial(cube_kernel, depth, main),
        out_shape=(
            jax.ShapeDtypeStruct(piece, half),
            jax.ShapeDtypeStruct((1, hidden), wide),
        ),
        in_specs=[vmem, vmem] + [anywhere] * 5 + [vmem],
        out_specs=(vmem, vmem),
        scratch_shapes=[
            pltpu.VMEM((2, shards, blocks) + piece, half),
            pltpu.VMEM((8, tok), wide),
            pltpu.VMEM((blocks, 8, tok), wide),
            pltpu.VMEM((blocks, slots, tok), half),
            pltpu.VMEM((blocks, tok, slots), half),
            pltpu.VMEM((blocks, slots, 1), wide),
            pltpu.VMEM((count, feat), half),
            pltpu.VMEM((count, hidden), wide),
            pltpu.VMEM((count, hidden), wide),
            pltpu.VMEM((count, hidden), wide),
            pltpu.VMEM((PAIR, 2, feat, hidden), half),
            pltpu.VMEM((PAIR, hidden, feat), half),
            pltpu.VMEM((ROW_TILE, hidden), wide),
            pltpu.VMEM((count, hidden), half),
            pltpu.VMEM((count, hidden), half),
            pltpu.VMEM((blocks, slots, feat), half),
            pltpu.VMEM((shards, PAIR) + piece, half),
            pltpu.VMEM((shards,) + piece, wide),
            pltpu.VMEM((shards,) + piece, half),
            pltpu.VMEM((depth,) + piece, half),
            pltpu.VMEM((depth,) + piece, half),
            pltpu.VMEM((depth,) + piece, half),
            dma((2,)),
            dma((PAIR, 2)),
            dma((PAIR,)),
            dma((3,)),
            dma((blocks,)),
            dma((2, 5, depth * blocks)),
            dma((2, shards, blocks)),
            dma((shards, PAIR)),
            dma((shards, PAIR)),
            dma((shards,)),
            dma((shards,)),
            dma((depth,)),
            dma((depth,)),
            dma((depth,)),
            dma((2, depth)),
        ],
        compiler_params=pltpu.CompilerParams(
            collective_id=2, has_side_effects=True, vmem_limit_bytes=VMEM_LIMIT
        ),
    )(expert_ids, combine, tokens, cotangent, gate_w, up_w, down_w, scale)


def local_cube(
    depth, tokens, cotangent, expert_ids, combine, w_gate, w_up, w_down, scale_vector
):
    return cube(
        depth, expert_ids, combine, tokens, cotangent, w_gate[0], w_up[0], w_down[0], scale_vector
    )


def local(ring, tokens, cotangent, expert_ids, combine, w_gate, w_up, w_down, scale_vector):
    experts = lax.axis_size("expert")
    tok_count = tokens.shape[0]
    capacity = 2 * tok_count // experts + 1
    dispatch, slot_weight, slot_ids = route_tables(
        expert_ids[None], combine[None], experts, capacity
    )
    dispatch_half = dispatch[0].astype(jnp.bfloat16)
    slot_weight = slot_weight[0]
    flat_index = expert_ids * capacity + slot_ids[0]
    sent_rows = jnp.einsum(
        "ect,td->ecd", dispatch_half, tokens, preferred_element_type=jnp.float32
    ).astype(jnp.bfloat16)
    cot_rows = jnp.einsum(
        "ect,td->ecd", dispatch_half, cotangent, preferred_element_type=jnp.float32
    )
    sent_grads = (slot_weight[:, :, None] * cot_rows).astype(jnp.bfloat16)
    sent = jnp.concatenate([sent_rows, sent_grads], axis=2)
    got = lax.all_to_all(sent, "expert", split_axis=0, concat_axis=0, tiled=True)
    row_count = experts * capacity
    padding = -row_count % ROW_TILE
    x = jnp.pad(got.reshape(row_count, got.shape[2]), ((0, padding), (0, 0)))
    gate_w = w_gate[0]
    up_w = w_up[0]
    down_w = w_down[0]
    gate_act, up_act, grads = gather_acts(ring, x, gate_w, up_w)
    hidden_grad = lax.dot_general(
        grads, down_w, (((1,), (1,)), ((), ())), preferred_element_type=jnp.float32
    )
    sigmoid_gate = jax.nn.sigmoid(gate_act)
    silu_gate = gate_act * sigmoid_gate
    scale_grad = jnp.sum(hidden_grad * silu_gate * up_act, axis=0)
    scaled_grad = hidden_grad * scale_vector[0]
    up_grad = (scaled_grad * silu_gate).astype(jnp.bfloat16)
    gate_grad = (
        scaled_grad * up_act * sigmoid_gate * (1.0 + gate_act * (1.0 - sigmoid_gate))
    ).astype(jnp.bfloat16)
    halves = scatter_rows(ring, gate_grad, up_grad, gate_w, up_w)
    summed = jnp.concatenate([halves[0], halves[1]], axis=1)[:row_count]
    slot_part = summed.reshape(experts, capacity, summed.shape[1])
    returned = lax.all_to_all(slot_part, "expert", split_axis=0, concat_axis=0, tiled=True)
    token_grads = combine_slots(returned.reshape(row_count, returned.shape[2]), flat_index)
    return (token_grads.astype(jnp.bfloat16), scale_grad[None, :])


def solution(mesh):
    placed = (
        P("expert", "dp"),
        P("expert", "dp"),
        P("expert", None),
        P("expert", None),
        P("expert", None, "dp"),
        P("expert", None, "dp"),
        P("expert", "dp", None),
        P("expert", "dp"),
    )
    count = mesh.shape["dp"]
    depth = 1 + max(k for _, k, _ in FRONT_PLAN)
    if mesh.shape["expert"] == PAIR * PAIR and count == PAIR * depth:
        body = functools.partial(local_cube, depth)
    else:
        body = functools.partial(local, ring_order(mesh))
    return jax.shard_map(
        body,
        mesh=mesh,
        in_specs=placed,
        out_specs=(P("expert", "dp"), P("expert", "dp")),
        check_vma=False,
    )
```
